32 devices in a mesh: groups: 2 (over y), seq: 4 (over z), head: 2 (over x), layer: 2 (over core).
Axes of the slice: x: 2, y: 2, z: 4, core: 2. Of those that a mesh axis runs over, the one named last changes fastest.
Arguments:
- kv_cache: bfloat16 [2, 2, 8, 4096, 2, 128], P(None, 'layer', 'groups', 'seq', 'head'), parts along dimension 2, may hold values from -800 to 800
- valid_blocks: int32 [8], P('groups'), parts along dimension 0, may hold values from 1 to 32, 64 in all
Outputs:
- decode_cache: bfloat16 [2, 2, 8, 4096, 2, 128], P(None, 'layer', ('groups', 'seq'), None, 'head'), parts along dimension 2
- centers: float32 [2, 2, 8, 2, 128], P(None, 'layer', 'groups', 'head'), parts along dimension 2
- scales: float32 [2, 2, 8, 2, 128], P(None, 'layer', 'groups', 'head'), parts along dimension 2
The draws below stay inside these ranges and needn't reach their ends.
There are 2 independent parts, one for each index of `groups`. The reference program is written for one: setup_inputs(seed, part) draws one part's arguments, and reference() takes and returns one part's arrays. A program takes and returns all parts, laid end to end along the dimension named above; each array names one. Nothing has to cross between parts.
Inputs may be any that keep to these rules, and one draw needn't show every extreme that they name: `valid_blocks`: the counts of the 4 users sum to 64, and the largest equals 32.
All inputs are finite; a program needn't handle non-finite values.
Results may differ from the reference program's by a relative error of at most 0.001.
Values may be sent and summed in bfloat16 or wider, within the bound.
A program may use at most 64 MiB of HBM per device.

```python
import math
import jax
import jax.numpy as jnp
import numpy as np

HEAD = 128
KVH = 2
LAYERS = 2
USERS = 4
PDEV = 1024
BLOCK = 128
SEQ = 4096
NBLK = 32
N_SEQ = 4


def draw_kv_cache(key, part):
    shape = (2, LAYERS, USERS, SEQ, KVH, HEAD)
    row_shape = (2, LAYERS, USERS, SEQ, KVH, 1)
    col_shape = (2, LAYERS, USERS, 1, KVH, HEAD)
    keys = jax.random.split(jax.random.fold_in(key, 11), 4)
    cols = jnp.exp(jax.random.uniform(keys[1], col_shape, jnp.float32, 0.0, math.log(10.0)))
    trend = 1.0 + 2.0 * jnp.arange(SEQ, dtype=jnp.float32).reshape(1, 1, 1, SEQ, 1, 1) / SEQ
    rows = jnp.exp(jax.random.uniform(keys[0], row_shape, jnp.float32, 0.0, math.log(10.0)))
    noise = jnp.clip(jax.random.normal(keys[2], shape, jnp.float32), -4.0, 4.0)
    offset = jnp.clip(jax.random.normal(keys[3], col_shape, jnp.float32), -4.0, 4.0) * 3.0 * cols
    value = trend * (offset + 0.3 * rows * cols * noise)
    return value.astype(jnp.bfloat16)


def split_up(amount, total, reach, skew):
    portions = [(1 << 20) // math.isqrt(standing ** skew) + 1 for standing in range(2, amount + 1)]
    spare, counts = total - reach - (amount - 1), [1] * (amount - 1)
    while spare > 0:
        candidates = [i for i in range(amount - 1) if counts[i] < reach]
        pool, remaining = sum([portions[i] for i in candidates]), spare
        for i in candidates:
            more = min(reach - counts[i], max(1, remaining * portions[i] // pool), spare)
            counts[i] = counts[i] + more
            spare = spare - more
    return np.array([reach] + counts)


def uneven_parts(key, count, total, limit, lean):
    if count == 2:
        one = jax.random.randint(key, (), max(1, total - limit), min(limit, total - 1) + 1)
        return jnp.stack([one, total - one])
    sizes = jnp.asarray(split_up(count, total, limit, lean), jnp.int32)
    pairs = (count - 1) // 2
    donor, sink = sizes[1:1 + 2 * pairs:2], sizes[2:2 + 2 * pairs:2]
    margin = jnp.minimum(donor - 1, limit - sink)
    shifted = jax.random.randint(jax.random.fold_in(key, 1), (pairs,), 0, 1 << 20) % (margin + 1)
    sizes = sizes.at[1:1 + 2 * pairs:2].set(donor - shifted).at[2:2 + 2 * pairs:2].set(sink + shifted)
    return sizes[jax.random.permutation(jax.random.fold_in(key, 2), count)]


def setup_inputs(seed: int = 0, part: int = 0) -> dict:
    key_list = jax.random.split(jax.random.key(seed), 3)
    part_keys = jax.random.split(jax.random.fold_in(key_list[2], part), 3)
    return {
        "kv_cache": draw_kv_cache(jax.random.fold_in(jax.random.fold_in(key_list[2], part), 71), part),
        "valid_blocks": uneven_parts(part_keys[1], USERS, USERS * NBLK // 2, NBLK, 2).astype(jnp.int32),
    }


epsilon = 1e-6


def reference(kv_cache, valid_blocks):
    lengths = valid_blocks.astype(jnp.int32) * BLOCK
    values = kv_cache.astype(jnp.float32)
    position = jnp.arange(SEQ, dtype=jnp.int32)
    is_live = position[None, :] < lengths[:, None]
    live_mask = is_live[None, None, :, :, None, None]
    totals = jnp.sum(jnp.where(live_mask, values, 0.0), axis=3)
    centers = totals / lengths.astype(jnp.float32)[None, None, :, None, None]
    spread = jnp.max(jnp.where(live_mask, jnp.abs(values - centers[:, :, :, None]), 0.0), axis=3)
    scales = spread + epsilon
    normed = jnp.where(live_mask, (values - centers[:, :, :, None]) / scales[:, :, :, None], 0.0).astype(jnp.bfloat16)
    owns = N_SEQ // USERS
    slice_len = PDEV // owns
    shaped = normed.reshape(2, LAYERS, USERS, N_SEQ, owns, slice_len, KVH, HEAD)
    shaped = jnp.transpose(shaped, (0, 1, 2, 4, 3, 5, 6, 7))
    decode_cache = shaped.reshape(2, LAYERS, USERS * owns, N_SEQ * slice_len, KVH, HEAD)
    return decode_cache, centers, scales
```

```python
import functools

import jax
import jax.numpy as jnp
from jax import lax
from jax.experimental import pallas as pl
from jax.experimental.pallas import tpu as pltpu
from jax.sharding import PartitionSpec as P

BLOCK = 128
ROWS = 8
CHUNK = 256
GRANT = 16 * 2**20
EPSILON = 1e-06


def normalised(recv_ref, k, rows, first, length, center, inverse):
    x = recv_ref[k, rows, :].astype(jnp.float32)
    position = first + lax.broadcasted_iota(jnp.int32, x.shape, 0)
    return jnp.where(position < length, (x - center) * inverse, 0.0).astype(jnp.bfloat16)


def transport(n, quarter, chunk, blocks_ref, kv_ref, recv_ref, centers_ref, scales_ref,
              inverse_ref, stats_ref, blocks, local, load_sem, blocks_sem, own_sem, send_sem, recv_sem,
              stat_send, stat_recv, ready):
    kinds, users, per_dev, width = kv_ref.shape
    part = per_dev // quarter
    pieces = part // chunk
    me = lax.axis_index("seq")
    mids = (n // 2 - 1, n // 2)
    mid = (me == mids[0]) | (me == mids[1])
    outer = (me < mids[0]) | (me > mids[1])

    load = pltpu.make_async_copy(kv_ref, local, load_sem)
    load.start()
    fetch = pltpu.make_async_copy(blocks_ref, blocks, blocks_sem)
    fetch.start()

    barrier = pltpu.get_barrier_semaphore()
    for d in range(n):
        greets = (mid if d in mids else me >= 0) & (me != d)

        @pl.when(greets)
        def _():
            pl.semaphore_signal(barrier, inc=1, device_id={"seq": d})

    @pl.when(mid)
    def _():
        pl.semaphore_wait(barrier, 1)

    @pl.when(outer)
    def _():
        pl.semaphore_wait(barrier, n - 1)
        for d in mids:
            pl.semaphore_signal(ready, inc=1, device_id={"seq": d})

    def bulk(source, target, k, i):
        user, q = target // quarter, target % quarter
        return pltpu.make_async_remote_copy(
            src_ref=kv_ref.at[k, user, pl.ds(pl.multiple_of(q * part + i * chunk, chunk), chunk), :],
            dst_ref=recv_ref.at[k, pl.ds(pl.multiple_of(source * part + i * chunk, chunk), chunk), :],
            send_sem=send_sem.at[target, k, i],
            recv_sem=recv_sem.at[source, k, i],
            device_id={"seq": target},
        )

    def stat(source, target):
        return pltpu.make_async_remote_copy(
            src_ref=stats_ref.at[source],
            dst_ref=stats_ref.at[source],
            send_sem=stat_send.at[target],
            recv_sem=stat_recv.at[source],
            device_id={"seq": target},
        )

    def start_bulk(target, k):
        for i in range(pieces):
            bulk(me, target, k, i).start()

    early = jnp.where(mid, n - 1 - me, jnp.where(me < mids[0], n - 1, 0))
    start_bulk(early, 0)

    own = pltpu.make_async_copy(
        kv_ref.at[:, me // quarter, pl.ds(pl.multiple_of((me % quarter) * part, part), part), :],
        recv_ref.at[:, pl.ds(pl.multiple_of(me * part, part), part), :],
        own_sem,
    )
    own.start()
    fetch.wait()
    load.wait()

    count = per_dev // BLOCK
    for k in range(kinds):
        for u in range(users):
            live = blocks[u] - me * count

            def step(b, carry, k=k, u=u, live=live):
                total, high, low = carry
                x = local[k, u, pl.ds(pl.multiple_of(b * BLOCK, BLOCK), BLOCK), :].astype(jnp.float32)
                x = x.reshape(BLOCK // ROWS, ROWS, width)
                on = b < live
                total = total + jnp.where(on, jnp.sum(x, axis=0), 0.0)
                high = jnp.maximum(high, jnp.where(on, jnp.max(x, axis=0), -jnp.inf))
                low = jnp.minimum(low, jnp.where(on, jnp.min(x, axis=0), jnp.inf))
                return total, high, low

            shape = (ROWS, width)
            total, high, low = lax.fori_loop(
                0, count, step,
                (jnp.zeros(shape, jnp.float32), jnp.full(shape, -jnp.inf, jnp.float32),
                 jnp.full(shape, jnp.inf, jnp.float32)),
            )
            stats_ref[me, 0, k, u, :] = jnp.sum(total, axis=0)
            stats_ref[me, 1, k, u, :] = jnp.max(high, axis=0)
            stats_ref[me, 2, k, u, :] = jnp.min(low, axis=0)

    if n > 2:
        @pl.when(mid)
        def _():
            pl.semaphore_wait(ready, n - 2)

    for d in range(n):
        @pl.when(me != d)
        def _():
            stat(me, d).start()
    for dist in range(n - 1, 0, -1):
        for target, inside in ((me + dist, me + dist < n), (me - dist, me - dist >= 0)):
            for k in range(kinds):
                wanted = inside & (target != early) if k == 0 else inside

                @pl.when(wanted)
                def _():
                    start_bulk(target, k)

    for s in range(n):
        @pl.when(me != s)
        def _():
            stat(s, me).wait_recv()
    for u in range(users):
        length = (blocks[u] * BLOCK).astype(jnp.float32)
        for k in range(kinds):
            total = stats_ref[0, 0, k, u, :]
            high, low = stats_ref[0, 1, k, u, :], stats_ref[0, 2, k, u, :]
            for s in range(1, n):
                total = total + stats_ref[s, 0, k, u, :]
                high = jnp.maximum(high, stats_ref[s, 1, k, u, :])
                low = jnp.minimum(low, stats_ref[s, 2, k, u, :])
            center = total / jnp.full_like(total, length)
            scale = jnp.maximum(high - center, center - low) + EPSILON
            centers_ref[k, u, :] = center
            scales_ref[k, u, :] = scale
            inverse_ref[k, u, :] = 1.0 / scale

    user = me // quarter
    base = (me % quarter) * part
    length = jnp.zeros((1, width), jnp.int32)
    for u in range(users):
        length = jnp.where(user == u, blocks[u] * BLOCK, length)

    def normalise(source, k, i):
        center = centers_ref[k, pl.ds(user, 1), :]
        inverse = inverse_ref[k, pl.ds(user, 1), :]
        rows = pl.ds(pl.multiple_of(source * part + i * chunk, chunk), chunk)
        first = source * per_dev + base + i * chunk
        recv_ref[k, rows, :] = normalised(recv_ref, k, rows, first, length, center, inverse)

    def arrive(source, k):
        def step(i, _):
            bulk(source, me, k, i).wait_recv()
            normalise(source, k, i)
            return 0

        lax.fori_loop(0, pieces, step, 0)

    own.wait()
    for k in range(kinds):
        def step(i, _, k=k):
            normalise(me, k, i)
            return 0

        lax.fori_loop(0, pieces, step, 0)
    for dist in range(n - 1, 0, -1):
        for source, inside in ((me + dist, me + dist < n), (me - dist, me - dist >= 0)):
            late = mid & (source == n - 1 - me) if dist == 1 else me < 0
            for k in range(kinds):
                @pl.when(inside & ~late)
                def _():
                    arrive(source, k)

    @pl.when(mid)
    def _():
        for k in range(kinds):
            arrive(n - 1 - me, k)

    for s in range(n):
        @pl.when(me != s)
        def _():
            stat(me, s).wait_send()
            for k in range(kinds):
                for i in range(pieces):
                    bulk(me, s, k, i).wait_send()


def finish(recv_ref, c_ref, s_ref, out_ref, centers_ref, scales_ref, sems):
    copies = [
        pltpu.make_async_copy(recv_ref, out_ref, sems.at[0]),
        pltpu.make_async_copy(c_ref, centers_ref, sems.at[1]),
        pltpu.make_async_copy(s_ref, scales_ref, sems.at[2]),
    ]
    for copy in copies:
        copy.start()
    for copy in copies:
        copy.wait()


def on_device(kv_cache, valid_blocks):
    kind_count, layer_dev, user_count, per_dev, heads_dev, width = kv_cache.shape
    n = lax.axis_size("seq")
    quarter = n // user_count
    part = per_dev // quarter
    kinds = kind_count * layer_dev * heads_dev
    kv = jnp.transpose(kv_cache, (0, 1, 4, 2, 3, 5)).reshape(kinds, user_count, per_dev, width)
    kv = pltpu.with_memory_space_constraint(kv, pltpu.HBM)
    blocks = pltpu.with_memory_space_constraint(valid_blocks, pltpu.HBM)
    vmem = pl.BlockSpec(memory_space=pltpu.VMEM)
    smem = pl.BlockSpec(memory_space=pltpu.SMEM)
    anywhere = pl.BlockSpec(memory_space=pl.ANY)
    hbm = pl.BlockSpec(memory_space=pltpu.HBM)
    chunk = min(part, CHUNK)
    small = jax.ShapeDtypeStruct((kinds, user_count, width), jnp.float32)
    recv, centers, scales = pl.pallas_call(
        functools.partial(transport, n, quarter, chunk),
        out_shape=(
            jax.ShapeDtypeStruct((kinds, n * part, width), jnp.bfloat16),
            small,
            small,
        ),
        in_specs=[hbm, hbm],
        out_specs=(vmem,) * 3,
        scratch_shapes=[
            pltpu.VMEM((kinds, user_count, width), jnp.float32),
            pltpu.VMEM((n, 3, kinds, user_count, width), jnp.float32),
            pltpu.SMEM((user_count,), jnp.int32),
            pltpu.VMEM((kinds, user_count, per_dev, width), jnp.bfloat16),
            pltpu.SemaphoreType.DMA,
            pltpu.SemaphoreType.DMA,
            pltpu.SemaphoreType.DMA,
            pltpu.SemaphoreType.DMA((n, kinds, part // chunk)),
            pltpu.SemaphoreType.DMA((n, kinds, part // chunk)),
            pltpu.SemaphoreType.DMA((n,)),
            pltpu.SemaphoreType.DMA((n,)),
            pltpu.SemaphoreType.REGULAR,
        ],
        compiler_params=pltpu.CompilerParams(
            collective_id=0, has_side_effects=True, vmem_limit_bytes=GRANT
        ),
        name="transport",
    )(blocks, kv)
    out, centers, scales = pl.pallas_call(
        finish,
        out_shape=(jax.ShapeDtypeStruct((kinds, n * part, width), jnp.bfloat16), small, small),
        in_specs=[vmem] * 3,
        out_specs=(anywhere, anywhere, anywhere),
        scratch_shapes=[pltpu.SemaphoreType.DMA((3,))],
        compiler_params=pltpu.CompilerParams(vmem_limit_bytes=GRANT),
        name="finish",
    )(recv, centers, scales)

    def spread(x, middle):
        x = x.reshape(kind_count, layer_dev, heads_dev, *middle, width)
        return jnp.moveaxis(x, 2, -2)

    return (
        spread(out, (1, n * part)),
        spread(centers, (user_count,)),
        spread(scales, (user_count,)),
    )


def solution(mesh):
    in_specs = (P(None, "layer", "groups", "seq", "head", None), P("groups"))
    out_specs = (
        P(None, "layer", ("groups", "seq"), None, "head", None),
        P(None, "layer", "groups", "head", None),
        P(None, "layer", "groups", "head", None),
    )
    return jax.shard_map(
        on_device, mesh=mesh, in_specs=in_specs, out_specs=out_specs, check_vma=False
    )
```

```python
import functools

import jax
import jax.numpy as jnp
from jax import lax
from jax.experimental import pallas as pl
from jax.experimental.pallas import tpu as pltpu
from jax.sharding import PartitionSpec as P

BLOCK = 128
ROWS = 8
CHUNK = 512
GRANT = 16 * 2**20
EPSILON = 1e-06


def normalised(recv_ref, k, rows, first, length, center, inverse):
    x = recv_ref[k, rows, :].astype(jnp.float32)
    position = first + lax.broadcasted_iota(jnp.int32, x.shape, 0)
    return jnp.where(position < length, (x - center) * inverse, 0.0).astype(jnp.bfloat16)


def transport(n, quarter, chunk, blocks_ref, kv_ref, recv_ref, centers_ref, scales_ref,
              inverse_ref, stats_ref, half_ref, full_ref, blocks, local, load_sem, blocks_sem, own_sem, send_sem, recv_sem,
              stat_send, stat_recv, half_send, half_recv, full_send, full_recv, ready):
    kinds, users, per_dev, width = kv_ref.shape
    part = per_dev // quarter
    pieces = part // chunk
    me = lax.axis_index("seq")
    mids = (n // 2 - 1, n // 2)
    mid = (me == mids[0]) | (me == mids[1])
    outer = (me < mids[0]) | (me > mids[1])
    side = me // (n // 2)

    load = pltpu.make_async_copy(kv_ref, local, load_sem)
    load.start()
    fetch = pltpu.make_async_copy(blocks_ref, blocks, blocks_sem)
    fetch.start()

    barrier = pltpu.get_barrier_semaphore()
    for d in range(n):
        greets = (mid if d in mids else me >= 0) & (me != d)

        @pl.when(greets)
        def _():
            pl.semaphore_signal(barrier, inc=1, device_id={"seq": d})

    @pl.when(mid)
    def _():
        pl.semaphore_wait(barrier, 1)

    @pl.when(outer)
    def _():
        pl.semaphore_wait(barrier, n - 1)
        for d in mids:
            pl.semaphore_signal(ready, inc=1, device_id={"seq": d})

    def bulk(source, target, k, i):
        user, q = target // quarter, target % quarter
        return pltpu.make_async_remote_copy(
            src_ref=kv_ref.at[k, user, pl.ds(pl.multiple_of(q * part + i * chunk, chunk), chunk), :],
            dst_ref=recv_ref.at[k, pl.ds(pl.multiple_of(source * part + i * chunk, chunk), chunk), :],
            send_sem=send_sem.at[target, k, i],
            recv_sem=recv_sem.at[source, k, i],
            device_id={"seq": target},
        )

    def stat(source, target):
        return pltpu.make_async_remote_copy(
            src_ref=stats_ref.at[source],
            dst_ref=stats_ref.at[source],
            send_sem=stat_send,
            recv_sem=stat_recv.at[source],
            device_id={"seq": target},
        )

    def across(origin):
        return pltpu.make_async_remote_copy(
            src_ref=half_ref.at[origin],
            dst_ref=half_ref.at[origin],
            send_sem=half_send,
            recv_sem=half_recv,
            device_id={"seq": n - 1 - me},
        )

    def handed(target):
        return pltpu.make_async_remote_copy(
            src_ref=full_ref,
            dst_ref=full_ref,
            send_sem=full_send.at[target],
            recv_sem=full_recv,
            device_id={"seq": target},
        )

    def start_bulk(target, k, chunks):
        for i in chunks:
            bulk(me, target, k, i).start()

    def combine(into, left, right):
        into[0] = left[0] + right[0]
        into[1] = jnp.maximum(left[1], right[1])
        into[2] = jnp.minimum(left[2], right[2])

    early = jnp.where(mid, n - 1 - me, jnp.where(me < mids[0], n - 1, 0))
    start_bulk(early, 0, range(1))

    @pl.when(outer)
    def _():
        start_bulk(early, 0, range(1, pieces))


    own = pltpu.make_async_copy(
        kv_ref.at[:, me // quarter, pl.ds(pl.multiple_of((me % quarter) * part, part), part), :],
        recv_ref.at[:, pl.ds(pl.multiple_of(me * part, part), part), :],
        own_sem,
    )
    own.start()
    fetch.wait()
    load.wait()

    count = per_dev // BLOCK
    for k in range(kinds):
        for u in range(users):
            live = blocks[u] - me * count

            def step(b, carry, k=k, u=u, live=live):
                total, high, low = carry
                x = local[k, u, pl.ds(pl.multiple_of(b * BLOCK, BLOCK), BLOCK), :].astype(jnp.float32)
                x = x.reshape(BLOCK // ROWS, ROWS, width)
                on = b < live
                total = total + jnp.where(on, jnp.sum(x, axis=0), 0.0)
                high = jnp.maximum(high, jnp.where(on, jnp.max(x, axis=0), -jnp.inf))
                low = jnp.minimum(low, jnp.where(on, jnp.min(x, axis=0), jnp.inf))
                return total, high, low

            shape = (ROWS, width)
            total, high, low = lax.fori_loop(
                0, count, step,
                (jnp.zeros(shape, jnp.float32), jnp.full(shape, -jnp.inf, jnp.float32),
                 jnp.full(shape, jnp.inf, jnp.float32)),
            )
            stats_ref[me, 0, k, u, :] = jnp.sum(total, axis=0)
            stats_ref[me, 1, k, u, :] = jnp.max(high, axis=0)
            stats_ref[me, 2, k, u, :] = jnp.min(low, axis=0)

    for h in range(2):
        @pl.when(outer & (side == h))
        def _():
            stat(me, mids[h]).start()

        @pl.when(mid & (side == h))
        def _():
            if n > 2:
                pl.semaphore_wait(ready, n - 2)
            inner = [s for s in range(n) if s // (n // 2) == h and s != mids[h]]
            half_ref[h] = stats_ref[mids[h]]
            for s in inner:
                stat(s, me).wait_recv()
                combine(half_ref.at[h], half_ref.at[h], stats_ref.at[s])
            across(h).start()

    for dist in range(n - 1, 0, -1):
        for target, inside in ((me + dist, me + dist < n), (me - dist, me - dist >= 0)):
            @pl.when(inside & (target != early))
            def _():
                start_bulk(target, 0, range(pieces))

            @pl.when(inside & (target == early) & mid)
            def _():
                start_bulk(target, 0, range(1, pieces))

            @pl.when(inside)
            def _():
                for k in range(1, kinds):
                    start_bulk(target, k, range(pieces))

    for h in range(2):
        @pl.when(mid & (side == h))
        def _():
            across(1 - h).wait_recv()
            combine(full_ref, half_ref.at[0], half_ref.at[1])
            for s in range(n):
                if s // (n // 2) == h and s != mids[h]:
                    handed(s).start()

    @pl.when(outer)
    def _():
        handed(me).wait_recv()

    for u in range(users):
        length = (blocks[u] * BLOCK).astype(jnp.float32)
        for k in range(kinds):
            total, high, low = full_ref[0, k, u, :], full_ref[1, k, u, :], full_ref[2, k, u, :]
            center = total / jnp.full_like(total, length)
            scale = jnp.maximum(high - center, center - low) + EPSILON
            centers_ref[k, u, :] = center
            scales_ref[k, u, :] = scale
            inverse_ref[k, u, :] = 1.0 / scale

    user = me // quarter
    base = (me % quarter) * part
    length = jnp.zeros((1, width), jnp.int32)
    for u in range(users):
        length = jnp.where(user == u, blocks[u] * BLOCK, length)

    def normalise(source, k, i):
        center = centers_ref[k, pl.ds(user, 1), :]
        inverse = inverse_ref[k, pl.ds(user, 1), :]
        rows = pl.ds(pl.multiple_of(source * part + i * chunk, chunk), chunk)
        first = source * per_dev + base + i * chunk
        recv_ref[k, rows, :] = normalised(recv_ref, k, rows, first, length, center, inverse)

    def arrive(source, k):
        def step(i, _):
            bulk(source, me, k, i).wait_recv()
            normalise(source, k, i)
            return 0

        lax.fori_loop(0, pieces, step, 0)

    own.wait()
    for k in range(kinds):
        def step(i, _, k=k):
            normalise(me, k, i)
            return 0

        lax.fori_loop(0, pieces, step, 0)
    for dist in range(n - 1, 0, -1):
        for source, inside in ((me + dist, me + dist < n), (me - dist, me - dist >= 0)):
            late = mid & (source == n - 1 - me) if dist == 1 else me < 0
            for k in range(kinds):
                @pl.when(inside & ~late)
                def _():
                    arrive(source, k)

    @pl.when(mid)
    def _():
        for k in range(kinds):
            arrive(n - 1 - me, k)

    for s in range(n):
        @pl.when(me != s)
        def _():
            for k in range(kinds):
                for i in range(pieces):
                    bulk(me, s, k, i).wait_send()

    for h in range(2):
        @pl.when(outer & (side == h))
        def _():
            stat(me, mids[h]).wait_send()

        @pl.when(mid & (side == h))
        def _():
            across(h).wait_send()
            for s in range(n):
                if s // (n // 2) == h and s != mids[h]:
                    handed(s).wait_send()


def finish(recv_ref, c_ref, s_ref, out_ref, centers_ref, scales_ref, sems):
    copies = [
        pltpu.make_async_copy(recv_ref, out_ref, sems.at[0]),
        pltpu.make_async_copy(c_ref, centers_ref, sems.at[1]),
        pltpu.make_async_copy(s_ref, scales_ref, sems.at[2]),
    ]
    for copy in copies:
        copy.start()
    for copy in copies:
        copy.wait()


def on_device(kv_cache, valid_blocks):
    kind_count, layer_dev, user_count, per_dev, heads_dev, width = kv_cache.shape
    n = lax.axis_size("seq")
    quarter = n // user_count
    part = per_dev // quarter
    kinds = kind_count * layer_dev * heads_dev
    kv = jnp.transpose(kv_cache, (0, 1, 4, 2, 3, 5)).reshape(kinds, user_count, per_dev, width)
    kv = pltpu.with_memory_space_constraint(kv, pltpu.HBM)
    blocks = pltpu.with_memory_space_constraint(valid_blocks, pltpu.HBM)
    vmem = pl.BlockSpec(memory_space=pltpu.VMEM)
    smem = pl.BlockSpec(memory_space=pltpu.SMEM)
    anywhere = pl.BlockSpec(memory_space=pl.ANY)
    hbm = pl.BlockSpec(memory_space=pltpu.HBM)
    chunk = min(part, CHUNK)
    small = jax.ShapeDtypeStruct((kinds, user_count, width), jnp.float32)
    recv, centers, scales = pl.pallas_call(
        functools.partial(transport, n, quarter, chunk),
        out_shape=(
            jax.ShapeDtypeStruct((kinds, n * part, width), jnp.bfloat16),
            small,
            small,
        ),
        in_specs=[hbm, hbm],
        out_specs=(vmem,) * 3,
        scratch_shapes=[
            pltpu.VMEM((kinds, user_count, width), jnp.float32),
            pltpu.VMEM((n, 3, kinds, user_count, width), jnp.float32),
            pltpu.VMEM((2, 3, kinds, user_count, width), jnp.float32),
            pltpu.VMEM((3, kinds, user_count, width), jnp.float32),
            pltpu.SMEM((user_count,), jnp.int32),
            pltpu.VMEM((kinds, user_count, per_dev, width), jnp.bfloat16),
            pltpu.SemaphoreType.DMA,
            pltpu.SemaphoreType.DMA,
            pltpu.SemaphoreType.DMA,
            pltpu.SemaphoreType.DMA((n, kinds, part // chunk)),
            pltpu.SemaphoreType.DMA((n, kinds, part // chunk)),
            pltpu.SemaphoreType.DMA,
            pltpu.SemaphoreType.DMA((n,)),
            pltpu.SemaphoreType.DMA,
            pltpu.SemaphoreType.DMA,
            pltpu.SemaphoreType.DMA((n,)),
            pltpu.SemaphoreType.DMA,
            pltpu.SemaphoreType.REGULAR,
        ],
        compiler_params=pltpu.CompilerParams(
            collective_id=0, has_side_effects=True, vmem_limit_bytes=GRANT
        ),
        name="transport",
    )(blocks, kv)
    out, centers, scales = pl.pallas_call(
        finish,
        out_shape=(jax.ShapeDtypeStruct((kinds, n * part, width), jnp.bfloat16), small, small),
        in_specs=[vmem] * 3,
        out_specs=(anywhere, anywhere, anywhere),
        scratch_shapes=[pltpu.SemaphoreType.DMA((3,))],
        compiler_params=pltpu.CompilerParams(vmem_limit_bytes=GRANT),
        name="finish",
    )(recv, centers, scales)

    def spread(x, middle):
        x = x.reshape(kind_count, layer_dev, heads_dev, *middle, width)
        return jnp.moveaxis(x, 2, -2)

    return (
        spread(out, (1, n * part)),
        spread(centers, (user_count,)),
        spread(scales, (user_count,)),
    )


def solution(mesh):
    in_specs = (P(None, "layer", "groups", "seq", "head", None), P("groups"))
    out_specs = (
        P(None, "layer", ("groups", "seq"), None, "head", None),
        P(None, "layer", "groups", "head", None),
        P(None, "layer", "groups", "head", None),
    )
    return jax.shard_map(
        on_device, mesh=mesh, in_specs=in_specs, out_specs=out_specs, check_vma=False
    )
```

```python
import functools

import jax
import jax.numpy as jnp
from jax import lax
from jax.experimental import pallas as pl
from jax.experimental.pallas import tpu as pltpu
from jax.sharding import PartitionSpec as P

BLOCK = 128
ROWS = 8
GRANT = 16 * 2**20
EPSILON = 1e-06


def normalised(recv_ref, k, rows, first, length, center, inverse):
    x = recv_ref[k, rows, :].astype(jnp.float32)
    position = first + lax.broadcasted_iota(jnp.int32, x.shape, 0)
    return jnp.where(position < length, (x - center) * inverse, 0.0).astype(jnp.bfloat16)


def transport(n, quarter, blocks_ref, kv_ref, recv_ref, centers_ref, scales_ref,
              inverse_ref, stats_ref, half_ref, full_ref, blocks, local, load_sem, blocks_sem, own_sem, send_sem, recv_sem, pair_send, pair_recv,
              stat_send, stat_recv, half_send, half_recv, full_send, full_recv, ready):
    kinds, users, per_dev, width = kv_ref.shape
    part = per_dev // quarter
    cuts = (0, 3 * part // 4, part)
    spans = tuple((a, b - a) for a, b in zip(cuts, cuts[1:]))
    me = lax.axis_index("seq")
    mids = (n // 2 - 1, n // 2)
    mid = (me == mids[0]) | (me == mids[1])
    outer = (me < mids[0]) | (me > mids[1])
    side = me // (n // 2)

    load = pltpu.make_async_copy(kv_ref, local, load_sem)
    load.start()
    fetch = pltpu.make_async_copy(blocks_ref, blocks, blocks_sem)
    fetch.start()

    barrier = pltpu.get_barrier_semaphore()
    for d in range(n):
        greets = (mid if d in mids else me >= 0) & (me != d)

        @pl.when(greets)
        def _():
            pl.semaphore_signal(barrier, inc=1, device_id={"seq": d})

    @pl.when(mid)
    def _():
        pl.semaphore_wait(barrier, 1)

    @pl.when(outer)
    def _():
        pl.semaphore_wait(barrier, n - 1)
        for d in mids:
            pl.semaphore_signal(ready, inc=1, device_id={"seq": d})

    partner = n - 1 - me

    def copy(src, source, target, k, start, rows, sems):
        user, q = target // quarter, target % quarter
        unit = part // 4
        return pltpu.make_async_remote_copy(
            src_ref=src.at[k, user, pl.ds(pl.multiple_of(q * part + start, unit), rows), :],
            dst_ref=recv_ref.at[k, pl.ds(pl.multiple_of(source * part + start, unit), rows), :],
            send_sem=sems[0],
            recv_sem=sems[1],
            device_id={"seq": target},
        )

    def bulk(source, target, k, src=local):
        return copy(src, source, target, k, 0, part, (send_sem.at[target, k], recv_sem.at[source, k]))

    def pair(source, target, k, i, src=local):
        start, rows = spans[i]
        return copy(src, source, target, k, start, rows, (pair_send.at[k, i], pair_recv.at[k, i]))

    def stat(source, target):
        return pltpu.make_async_remote_copy(
            src_ref=stats_ref.at[source],
            dst_ref=stats_ref.at[source],
            send_sem=stat_send,
            recv_sem=stat_recv.at[source],
            device_id={"seq": target},
        )

    def across(origin):
        return pltpu.make_async_remote_copy(
            src_ref=half_ref.at[origin],
            dst_ref=half_ref.at[origin],
            send_sem=half_send,
            recv_sem=half_recv,
            device_id={"seq": n - 1 - me},
        )

    def handed(target):
        return pltpu.make_async_remote_copy(
            src_ref=full_ref,
            dst_ref=full_ref,
            send_sem=full_send.at[target],
            recv_sem=full_recv,
            device_id={"seq": target},
        )

    def combine(into, left, right):
        into[0] = left[0] + right[0]
        into[1] = jnp.maximum(left[1], right[1])
        into[2] = jnp.minimum(left[2], right[2])

    early = jnp.where(me < mids[0], n - 1, 0)

    @pl.when(mid)
    def _():
        pair(me, partner, 0, 0, kv_ref).start()

    @pl.when(outer)
    def _():
        bulk(me, early, 0, kv_ref).start()

    own = pltpu.make_async_copy(
        kv_ref.at[:, me // quarter, pl.ds(pl.multiple_of((me % quarter) * part, part), part), :],
        recv_ref.at[:, pl.ds(pl.multiple_of(me * part, part), part), :],
        own_sem,
    )
    own.start()
    fetch.wait()
    load.wait()

    count = per_dev // BLOCK
    for k in range(kinds):
        for u in range(users):
            live = blocks[u] - me * count

            def step(b, carry, k=k, u=u, live=live):
                total, high, low = carry
                x = local[k, u, pl.ds(pl.multiple_of(b * BLOCK, BLOCK), BLOCK), :].astype(jnp.float32)
                x = x.reshape(BLOCK // ROWS, ROWS, width)
                on = b < live
                total = total + jnp.where(on, jnp.sum(x, axis=0), 0.0)
                high = jnp.maximum(high, jnp.where(on, jnp.max(x, axis=0), -jnp.inf))
                low = jnp.minimum(low, jnp.where(on, jnp.min(x, axis=0), jnp.inf))
                return total, high, low

            shape = (ROWS, width)
            total, high, low = lax.fori_loop(
                0, count, step,
                (jnp.zeros(shape, jnp.float32), jnp.full(shape, -jnp.inf, jnp.float32),
                 jnp.full(shape, jnp.inf, jnp.float32)),
            )
            stats_ref[me, 0, k, u, :] = jnp.sum(total, axis=0)
            stats_ref[me, 1, k, u, :] = jnp.max(high, axis=0)
            stats_ref[me, 2, k, u, :] = jnp.min(low, axis=0)

    for h in range(2):
        @pl.when(outer & (side == h))
        def _():
            stat(me, mids[h]).start()

        @pl.when(mid & (side == h))
        def _():
            if n > 2:
                pl.semaphore_wait(ready, n - 2)
            inner = [s for s in range(n) if s // (n // 2) == h and s != mids[h]]
            half_ref[h] = stats_ref[mids[h]]
            for s in inner:
                stat(s, me).wait_recv()
                combine(half_ref.at[h], half_ref.at[h], stats_ref.at[s])
            across(h).start()

    for dist in range(n - 1, 0, -1):
        for target, inside in ((me + dist, me + dist < n), (me - dist, me - dist >= 0)):
            paired = mid & (target == partner)
            for k in range(kinds):
                sent = outer & (target == early) if k == 0 else me < 0

                @pl.when(inside & ~paired & ~sent)
                def _():
                    bulk(me, target, k).start()

    @pl.when(mid)
    def _():
        for k in range(kinds):
            for i in range(len(spans)):
                if k + i > 0:
                    pair(me, partner, k, i).start()

    for h in range(2):
        @pl.when(mid & (side == h))
        def _():
            across(1 - h).wait_recv()
            combine(full_ref, half_ref.at[0], half_ref.at[1])
            for s in range(n):
                if s // (n // 2) == h and s != mids[h]:
                    handed(s).start()

    @pl.when(outer)
    def _():
        handed(me).wait_recv()

    for u in range(users):
        length = (blocks[u] * BLOCK).astype(jnp.float32)
        for k in range(kinds):
            total, high, low = full_ref[0, k, u, :], full_ref[1, k, u, :], full_ref[2, k, u, :]
            center = total / jnp.full_like(total, length)
            scale = jnp.maximum(high - center, center - low) + EPSILON
            centers_ref[k, u, :] = center
            scales_ref[k, u, :] = scale
            inverse_ref[k, u, :] = 1.0 / scale

    user = me // quarter
    base = (me % quarter) * part
    length = jnp.zeros((1, width), jnp.int32)
    for u in range(users):
        length = jnp.where(user == u, blocks[u] * BLOCK, length)

    def normalise(source, k, start, rows):
        center = centers_ref[k, pl.ds(user, 1), :]
        inverse = inverse_ref[k, pl.ds(user, 1), :]
        step = part // 4

        def at(i, _):
            here = start + i * step
            place = pl.ds(pl.multiple_of(source * part + here, step), step)
            first = source * per_dev + base + here
            recv_ref[k, place, :] = normalised(recv_ref, k, place, first, length, center, inverse)
            return 0

        lax.fori_loop(0, rows // step, at, 0)

    own.wait()
    for k in range(kinds):
        normalise(me, k, 0, part)
    for dist in range(n - 1, 0, -1):
        for source, inside in ((me + dist, me + dist < n), (me - dist, me - dist >= 0)):
            paired = mid & (source == partner)
            for k in range(kinds):
                @pl.when(inside & ~paired)
                def _():
                    bulk(source, me, k).wait_recv()
                    normalise(source, k, 0, part)

    @pl.when(mid)
    def _():
        for k in range(kinds):
            for i, (start, rows) in enumerate(spans):
                pair(partner, me, k, i).wait_recv()
                normalise(partner, k, start, rows)

    for s in range(n):
        paired = mid & (partner == s)

        @pl.when((me != s) & ~paired)
        def _():
            for k in range(kinds):
                bulk(me, s, k).wait_send()

    @pl.when(mid)
    def _():
        for k in range(kinds):
            for i in range(len(spans)):
                pair(me, partner, k, i).wait_send()

    for h in range(2):
        @pl.when(outer & (side == h))
        def _():
            stat(me, mids[h]).wait_send()

        @pl.when(mid & (side == h))
        def _():
            across(h).wait_send()
            for s in range(n):
                if s // (n // 2) == h and s != mids[h]:
                    handed(s).wait_send()


def finish(recv_ref, c_ref, s_ref, out_ref, centers_ref, scales_ref, sems):
    copies = [
        pltpu.make_async_copy(recv_ref, out_ref, sems.at[0]),
        pltpu.make_async_copy(c_ref, centers_ref, sems.at[1]),
        pltpu.make_async_copy(s_ref, scales_ref, sems.at[2]),
    ]
    for copy in copies:
        copy.start()
    for copy in copies:
        copy.wait()


def on_device(kv_cache, valid_blocks):
    kind_count, layer_dev, user_count, per_dev, heads_dev, width = kv_cache.shape
    n = lax.axis_size("seq")
    quarter = n // user_count
    part = per_dev // quarter
    kinds = kind_count * layer_dev * heads_dev
    kv = jnp.transpose(kv_cache, (0, 1, 4, 2, 3, 5)).reshape(kinds, user_count, per_dev, width)
    kv = pltpu.with_memory_space_constraint(kv, pltpu.HBM)
    blocks = pltpu.with_memory_space_constraint(valid_blocks, pltpu.HBM)
    vmem = pl.BlockSpec(memory_space=pltpu.VMEM)
    smem = pl.BlockSpec(memory_space=pltpu.SMEM)
    anywhere = pl.BlockSpec(memory_space=pl.ANY)
    hbm = pl.BlockSpec(memory_space=pltpu.HBM)
    small = jax.ShapeDtypeStruct((kinds, user_count, width), jnp.float32)
    recv, centers, scales = pl.pallas_call(
        functools.partial(transport, n, quarter),
        out_shape=(
            jax.ShapeDtypeStruct((kinds, n * part, width), jnp.bfloat16),
            small,
            small,
        ),
        in_specs=[hbm, hbm],
        out_specs=(vmem,) * 3,
        scratch_shapes=[
            pltpu.VMEM((kinds, user_count, width), jnp.float32),
            pltpu.VMEM((n, 3, kinds, user_count, width), jnp.float32),
            pltpu.VMEM((2, 3, kinds, user_count, width), jnp.float32),
            pltpu.VMEM((3, kinds, user_count, width), jnp.float32),
            pltpu.SMEM((user_count,), jnp.int32),
            pltpu.VMEM((kinds, user_count, per_dev, width), jnp.bfloat16),
            pltpu.SemaphoreType.DMA,
            pltpu.SemaphoreType.DMA,
            pltpu.SemaphoreType.DMA,
            pltpu.SemaphoreType.DMA((n, kinds)),
            pltpu.SemaphoreType.DMA((n, kinds)),
            pltpu.SemaphoreType.DMA((kinds, 2)),
            pltpu.SemaphoreType.DMA((kinds, 2)),
            pltpu.SemaphoreType.DMA,
            pltpu.SemaphoreType.DMA((n,)),
            pltpu.SemaphoreType.DMA,
            pltpu.SemaphoreType.DMA,
            pltpu.SemaphoreType.DMA((n,)),
            pltpu.SemaphoreType.DMA,
            pltpu.SemaphoreType.REGULAR,
        ],
        compiler_params=pltpu.CompilerParams(
            collective_id=0, has_side_effects=True, vmem_limit_bytes=GRANT
        ),
        name="transport",
    )(blocks, kv)
    out, centers, scales = pl.pallas_call(
        finish,
        out_shape=(jax.ShapeDtypeStruct((kinds, n * part, width), jnp.bfloat16), small, small),
        in_specs=[vmem] * 3,
        out_specs=(anywhere, anywhere, anywhere),
        scratch_shapes=[pltpu.SemaphoreType.DMA((3,))],
        compiler_params=pltpu.CompilerParams(vmem_limit_bytes=GRANT),
        name="finish",
    )(recv, centers, scales)

    def spread(x, middle):
        x = x.reshape(kind_count, layer_dev, heads_dev, *middle, width)
        return jnp.moveaxis(x, 2, -2)

    return (
        spread(out, (1, n * part)),
        spread(centers, (user_count,)),
        spread(scales, (user_count,)),
    )


def solution(mesh):
    in_specs = (P(None, "layer", "groups", "seq", "head", None), P("groups"))
    out_specs = (
        P(None, "layer", ("groups", "seq"), None, "head", None),
        P(None, "layer", "groups", "head", None),
        P(None, "layer", "groups", "head", None),
    )
    return jax.shard_map(
        on_device, mesh=mesh, in_specs=in_specs, out_specs=out_specs, check_vma=False
    )
```

```python
import functools

import jax
import jax.numpy as jnp
from jax import lax
from jax.experimental import pallas as pl
from jax.experimental.pallas import tpu as pltpu
from jax.sharding import PartitionSpec as P

BLOCK = 128
ROWS = 8
GRANT = 16 * 2**20
EPSILON = 1e-06
CLASSES = (
    (8, 8, 8, 8),
    (4, 8, 4, 8),
    (8, 4, 8, 4),
    (8, 2, 4, 8),
    (2, 8, 8, 4),
)


def classes(users):
    return tuple(c for c in CLASSES if len(c) == users) or ((8,) * users,)


def normalised(x, first, length, center, inverse):
    x = x.astype(jnp.float32)
    position = first + lax.broadcasted_iota(jnp.int32, x.shape, 0)
    return jnp.where(position < length, (x - center) * inverse, 0.0).astype(jnp.bfloat16)


def combine(into, left, right):
    into[0] = left[0] + right[0]
    into[1] = jnp.maximum(left[1], right[1])
    into[2] = jnp.minimum(left[2], right[2])


def each(low, high, action):
    def step(i, _):
        action(i)
        return 0

    lax.fori_loop(low, high, step, 0)


def gather(n, groups, quarter, blocks_ref, kv_ref, recv_ref, centers_ref, scales_ref, inverse_ref,
           lengths_ref, choice_ref, blocks, local, stats_ref, half_ref, full_ref,
           load_sem, fetch_sem, own_sem, send_sem, recv_sem, cut_send, cut_recv, stat_send, stat_recv,
           half_send, half_recv, full_send, full_recv, swap_send, swap_recv, ready):
    kinds, users, per_dev, width = kv_ref.shape
    part = per_dev // quarter
    half = n // 2
    me = lax.axis_index("seq")
    group = lax.axis_index("groups")
    mids = (half - 1, half)
    ends = (0, n - 1)
    mid = (me == mids[0]) | (me == mids[1])
    outer = (me < mids[0]) | (me > mids[1])
    side = me // half
    partner = n - 1 - me

    load = pltpu.make_async_copy(kv_ref, local, load_sem)
    load.start()
    fetch = pltpu.make_async_copy(blocks_ref, blocks.at[group], fetch_sem)
    fetch.start()

    barrier = pltpu.get_barrier_semaphore()
    for g in range(groups):
        @pl.when(group != g)
        def _():
            pl.semaphore_signal(barrier, inc=1, device_id={"groups": g})
    for d in range(n):
        greets = (mid if d in mids else me >= 0) & (me != d)

        @pl.when(greets)
        def _():
            pl.semaphore_signal(barrier, inc=1, device_id={"seq": d})

    @pl.when(mid)
    def _():
        pl.semaphore_wait(barrier, groups)

    @pl.when(outer)
    def _():
        pl.semaphore_wait(barrier, n + groups - 2)
        for d in mids:
            pl.semaphore_signal(ready, inc=1, device_id={"seq": d})

    def bulk(source, target, k):
        user, q = target // quarter, target % quarter
        return pltpu.make_async_remote_copy(
            src_ref=local.at[k, user, pl.ds(pl.multiple_of(q * part, part), part), :],
            dst_ref=recv_ref.at[k, pl.ds(pl.multiple_of(source * part, part), part), :],
            send_sem=send_sem.at[target, k],
            recv_sem=recv_sem.at[source, k],
            device_id={"seq": target},
        )

    def cut(source, target, k, i, src=local):
        user, q = target // quarter, target % quarter
        rows = part // 2
        return pltpu.make_async_remote_copy(
            src_ref=src.at[k, user, pl.ds(pl.multiple_of(q * part + i * rows, rows), rows), :],
            dst_ref=recv_ref.at[k, pl.ds(pl.multiple_of(source * part + i * rows, rows), rows), :],
            send_sem=cut_send.at[k, i],
            recv_sem=cut_recv.at[source, k, i],
            device_id={"seq": target},
        )

    def stat(source, target):
        return pltpu.make_async_remote_copy(
            src_ref=stats_ref.at[source],
            dst_ref=stats_ref.at[source],
            send_sem=stat_send,
            recv_sem=stat_recv.at[source],
            device_id={"seq": target},
        )

    def across(origin):
        return pltpu.make_async_remote_copy(
            src_ref=half_ref.at[origin],
            dst_ref=half_ref.at[origin],
            send_sem=half_send,
            recv_sem=half_recv,
            device_id={"seq": partner},
        )

    def handed(target):
        return pltpu.make_async_remote_copy(
            src_ref=full_ref,
            dst_ref=full_ref,
            send_sem=full_send.at[target],
            recv_sem=full_recv,
            device_id={"seq": target},
        )

    def swap(origin, g):
        return pltpu.make_async_remote_copy(
            src_ref=blocks.at[origin],
            dst_ref=blocks.at[origin],
            send_sem=swap_send.at[g],
            recv_sem=swap_recv.at[origin],
            device_id={"groups": g},
        )

    @pl.when(outer)
    def _():
        load.wait()

    for h in range(2):
        @pl.when(outer & (side == h))
        def _():
            cut(me, mids[1 - h], 0, 0, kv_ref).start()

    own = pltpu.make_async_copy(
        kv_ref.at[:, me // quarter, pl.ds(pl.multiple_of((me % quarter) * part, part), part), :],
        recv_ref.at[:, pl.ds(pl.multiple_of(me * part, part), part), :],
        own_sem,
    )
    own.start()
    fetch.wait()
    for g in range(groups):
        @pl.when(group != g)
        def _():
            swap(group, g).start()

    @pl.when(mid)
    def _():
        load.wait()

    for u in range(users):
        lengths_ref[pl.ds(u, 1), :] = jnp.full((1, width), blocks[group, u] * BLOCK, jnp.int32)
    count = per_dev // BLOCK
    for k in range(kinds):
        for u in range(users):
            live = blocks[group, u] - me * count

            def step(b, carry, k=k, u=u, live=live):
                total, high, low = carry
                x = local[k, u, pl.ds(pl.multiple_of(b * BLOCK, BLOCK), BLOCK), :].astype(jnp.float32)
                x = x.reshape(BLOCK // ROWS, ROWS, width)
                on = b < live
                total = total + jnp.where(on, jnp.sum(x, axis=0), 0.0)
                high = jnp.maximum(high, jnp.where(on, jnp.max(x, axis=0), -jnp.inf))
                low = jnp.minimum(low, jnp.where(on, jnp.min(x, axis=0), jnp.inf))
                return total, high, low

            shape = (ROWS, width)
            total, high, low = lax.fori_loop(
                0, count, step,
                (jnp.zeros(shape, jnp.float32), jnp.full(shape, -jnp.inf, jnp.float32),
                 jnp.full(shape, jnp.inf, jnp.float32)),
            )
            stats_ref[me, 0, k, u, :] = jnp.sum(total, axis=0)
            stats_ref[me, 1, k, u, :] = jnp.max(high, axis=0)
            stats_ref[me, 2, k, u, :] = jnp.min(low, axis=0)

    if n > 2:
        @pl.when(mid)
        def _():
            pl.semaphore_wait(ready, n - 2)

    odd = lax.axis_index("layer") % 2 == 1

    for h in range(2):
        halves = range(h * half, (h + 1) * half)
        others = [s for s in halves if s != ends[h]]
        there = [s for s in range(n) if s // half != h and s not in mids]

        @pl.when((side == h) & (me != ends[h]))
        def _():
            stat(me, ends[h]).start()

        @pl.when(outer & (me != ends[h]) & (side == h))
        def _():
            for k in range(kinds):
                for i in range(2):
                    if k + i:
                        cut(me, mids[1 - h], k, i).start()

        @pl.when(me == ends[h])
        def _():
            @pl.when(odd)
            def _():
                cut(me, mids[1 - h], 0, 1).start()

            half_ref[h] = stats_ref[ends[h]]
            for s in others:
                stat(s, me).wait_recv()
                combine(half_ref.at[h], half_ref.at[h], stats_ref.at[s])
            across(h).start()

            @pl.when(~odd)
            def _():
                cut(me, mids[1 - h], 0, 1).start()

            for k in range(1, kinds):
                cut(me, mids[1 - h], k, 0).start()

            @pl.when(odd)
            def _():
                for k in range(1, kinds):
                    cut(me, mids[1 - h], k, 1).start()

            across(1 - h).wait_recv()
            combine(full_ref, half_ref.at[0], half_ref.at[1])
            for s in others:
                handed(s).start()

            @pl.when(~odd)
            def _():
                for k in range(1, kinds):
                    cut(me, mids[1 - h], k, 1).start()

        for s in halves:
            @pl.when(me == s)
            def _():
                targets = (there if s not in mids else []) + [t for t in halves if t != s and t not in mids]
                for t in targets:
                    for k in range(kinds):
                        bulk(me, t, k).start()

    for g in range(groups):
        @pl.when(group != g)
        def _():
            swap(g, g).wait_recv()
    options = classes(users)
    choice = jnp.int32(0)
    for g in range(groups):
        pick = jnp.int32(0)
        for c, caps in enumerate(options):
            covers = None
            for u in range(users):
                source = mids[0] if u * quarter >= half else mids[1]
                most = source * per_dev + caps[u] * per_dev // 8
                fits = (blocks[g, u] * BLOCK <= most) if caps[u] < 8 else None
                if fits is not None:
                    covers = fits if covers is None else covers & fits
            pick = jnp.int32(c) if covers is None else jnp.where(covers, c, pick)
        choice = choice * len(options) + pick
    choice_ref[0] = choice

    @pl.when((me != ends[0]) & (me != ends[1]))
    def _():
        handed(me).wait_recv()

    for u in range(users):
        length = lengths_ref[u, :].astype(jnp.float32)
        for k in range(kinds):
            total, high, low = full_ref[0, k, u, :], full_ref[1, k, u, :], full_ref[2, k, u, :]
            center = total / length
            scale = jnp.maximum(high - center, center - low) + EPSILON
            centers_ref[k, u, :] = center
            scales_ref[k, u, :] = scale
            inverse_ref[k, u, :] = 1.0 / scale

    user = me // quarter
    base = (me % quarter) * part
    length = lengths_ref[pl.ds(user, 1), :]

    def normalise(source, k, rows):
        center = centers_ref[k, pl.ds(user, 1), :]
        inverse = inverse_ref[k, pl.ds(user, 1), :]
        step = part // 4

        def at(i):
            place = pl.ds(pl.multiple_of(source * part + i * step, step), step)
            first = source * per_dev + base + i * step
            recv_ref[k, place, :] = normalised(recv_ref[k, place, :], first, length, center, inverse)

        each(0, rows // step, at)

    own.wait()
    each(0, kinds, lambda k: normalise(me, k, part))

    def arrive(source):
        def at(k):
            bulk(source, me, k).wait_recv()
            normalise(source, k, part)

        each(0, kinds, at)

    for h in range(2):
        halves = range(h * half, (h + 1) * half)
        there = [s for s in range(n) if s // half != h and s not in mids]

        @pl.when(side == h)
        def _():
            @pl.when(outer)
            def _():
                for s in halves:
                    @pl.when(me != s)
                    def _():
                        arrive(s)

            for s in there:
                @pl.when(outer)
                def _():
                    arrive(s)

                @pl.when(mid)
                def _():
                    def at(k):
                        for i in range(2):
                            cut(s, me, k, i).wait_recv()
                        normalise(s, k, part)

                    each(0, kinds, at)

            for t in halves:
                if t not in mids:
                    @pl.when(me != t)
                    def _():
                        for k in range(kinds):
                            bulk(me, t, k).wait_send()

            @pl.when(outer)
            def _():
                for t in there:
                    for k in range(kinds):
                        bulk(me, t, k).wait_send()
                for k in range(kinds):
                    for i in range(2):
                        cut(me, mids[1 - h], k, i).wait_send()

            @pl.when(me != ends[h])
            def _():
                stat(me, ends[h]).wait_send()

            @pl.when(me == ends[h])
            def _():
                across(h).wait_send()
                for s in halves:
                    if s != ends[h]:
                        handed(s).wait_send()

    for g in range(groups):
        @pl.when(group != g)
        def _():
            swap(group, g).wait_send()


def remainder(index, n, groups, quarter, kv_ref, lengths_ref, centers_ref, inverse_ref, recv_ref,
              send_sem, recv_sem, near_send, near_recv, ready):
    kinds, users, per_dev, width = kv_ref.shape
    part = per_dev // quarter
    half = n // 2
    options = classes(users)
    me = lax.axis_index("seq")
    group = lax.axis_index("groups")
    mids = (half - 1, half)
    mid = (me == mids[0]) | (me == mids[1])
    outer = (me < mids[0]) | (me > mids[1])
    side = me // half

    barrier = pltpu.get_barrier_semaphore()
    for d in range(n):
        @pl.when(mid & (me != d))
        def _():
            pl.semaphore_signal(barrier, inc=1, device_id={"seq": d})

    @pl.when(mid)
    def _():
        pl.semaphore_wait(barrier, 1)

    @pl.when(outer)
    def _():
        pl.semaphore_wait(barrier, 2)
        for d in mids:
            pl.semaphore_signal(ready, inc=1, device_id={"seq": d})

    def window(target, caps):
        rows = caps[target // quarter] * per_dev // 8 - (target % quarter) * part
        return max(min(rows, part), 0)

    def late(target, caps, k):
        rows = window(target, caps)
        user, q = target // quarter, target % quarter
        return pltpu.make_async_remote_copy(
            src_ref=kv_ref.at[k, user, pl.ds(q * part, rows), :],
            dst_ref=recv_ref.at[k, pl.ds(0, rows), :],
            send_sem=send_sem.at[target, k],
            recv_sem=recv_sem.at[k],
            device_id={"seq": target},
        )

    def near(source, h, k):
        target = mids[h]
        user, q = target // quarter, target % quarter
        slot = 1 + (source if h == 0 else n - 1 - source)
        return pltpu.make_async_remote_copy(
            src_ref=kv_ref.at[k, user, pl.ds(q * part, part), :],
            dst_ref=recv_ref.at[k, pl.ds(slot * part, part), :],
            send_sem=near_send.at[k],
            recv_sem=near_recv.at[slot, k],
            device_id={"seq": target},
        )

    picks = []
    for g in reversed(range(groups)):
        picks.insert(0, options[index // len(options) ** (groups - 1 - g) % len(options)])

    def both(action):
        for g in range(groups):
            @pl.when(group == g)
            def _():
                action(picks[g])

    for h in range(2):
        for s in range(h * half, (h + 1) * half):
            if s not in mids:
                @pl.when(me == s)
                def _():
                    for k in range(kinds):
                        near(s, h, k).start()

    def split(h, caps):
        return kinds if 2 * window(mids[1 - h], caps) <= part else 1

    def send(targets, caps, which):
        for t in targets:
            for k in which:
                if window(t, caps):
                    late(t, caps, k).start()

    for h in range(2):
        away = [t for t in range(n) if t // half != h and t not in mids]

        @pl.when(me == mids[h])
        def _():
            both(lambda caps: send([mids[1 - h]], caps, range(split(h, caps))))
            if n > 2:
                pl.semaphore_wait(ready, n - 2)
            both(lambda caps: (
                send(away, caps, range(kinds)),
                send([mids[1 - h]], caps, range(split(h, caps), kinds)),
            ))

    user = me // quarter
    base = (me % quarter) * part
    length = lengths_ref[pl.ds(user, 1), :]
    step = part // 4

    def put(slot, source, k, i):
        center = centers_ref[k, pl.ds(user, 1), :]
        inverse = inverse_ref[k, pl.ds(user, 1), :]
        place = pl.ds(pl.multiple_of(slot * part + i * step, step), step)
        first = source * per_dev + base + i * step
        recv_ref[k, place, :] = normalised(recv_ref[k, place, :], first, length, center, inverse)

    def clear(k, i):
        recv_ref[k, pl.ds(pl.multiple_of(i * step, step), step), :] = jnp.zeros((step, width), jnp.bfloat16)

    for h in range(2):
        @pl.when(mid & (side == h))
        def _():
            for s in range(h * half, (h + 1) * half):
                if s not in mids:
                    slot = 1 + (s if h == 0 else n - 1 - s)
                    for k in range(kinds):
                        near(s, h, k).wait_recv()
                    each(0, kinds, lambda k: each(0, part // step, lambda i: put(slot, s, k, i)))

    def settle(t, caps):
        source = mids[1 - t // half]
        rows = window(t, caps)
        for k in range(kinds):
            each(rows // step, part // step, lambda i: clear(k, i))
        for k in range(kinds):
            if rows:
                late(t, caps, k).wait_recv()
                each(0, rows // step, lambda i: put(0, source, k, i))

    for t in range(n):
        @pl.when(me == t)
        def _():
            both(lambda caps: settle(t, caps))

    def drain(targets, caps):
        for t in targets:
            for k in range(kinds):
                if window(t, caps):
                    late(t, caps, k).wait_send()

    for h in range(2):
        away = [t for t in range(n) if t // half != h]

        @pl.when(me == mids[h])
        def _():
            both(lambda caps: drain(away, caps))

        for s in range(h * half, (h + 1) * half):
            if s not in mids:
                @pl.when(me == s)
                def _():
                    for k in range(kinds):
                        near(s, h, k).wait_send()


def finish(n, part, early_ref, late_ref, c_ref, s_ref, out_ref, centers_ref, scales_ref, sems):
    half = n // 2
    mids = (half - 1, half)
    me = lax.axis_index("seq")
    for t in range(n):
        @pl.when(me == t)
        def _():
            h = t // half
            pieces = []
            for s in range(n):
                at = s * part
                if s == mids[1 - h]:
                    pieces.append((late_ref, 0, at, part))
                elif t in mids and s != t and s // half == h:
                    pieces.append((late_ref, (1 + (s if h == 0 else n - 1 - s)) * part, at, part))
                elif pieces and pieces[-1][0] is early_ref:
                    _, a, b, rows = pieces.pop()
                    pieces.append((early_ref, a, b, rows + part))
                else:
                    pieces.append((early_ref, at, at, part))
            copies = [
                pltpu.make_async_copy(
                    ref.at[:, pl.ds(a, rows), :], out_ref.at[:, pl.ds(b, rows), :], sems.at[i])
                for i, (ref, a, b, rows) in enumerate(pieces)
            ] + [
                pltpu.make_async_copy(c_ref, centers_ref, sems.at[n]),
                pltpu.make_async_copy(s_ref, scales_ref, sems.at[n + 1]),
            ]
            for copy in copies:
                copy.start()
            for copy in copies:
                copy.wait()


def on_device(kv_cache, valid_blocks):
    kind_count, layer_dev, user_count, per_dev, heads_dev, width = kv_cache.shape
    n, groups = lax.axis_size("seq"), lax.axis_size("groups")
    quarter = n // user_count
    part = per_dev // quarter
    kinds = kind_count * layer_dev * heads_dev
    kv = jnp.transpose(kv_cache, (0, 1, 4, 2, 3, 5)).reshape(kinds, user_count, per_dev, width)
    kv = pltpu.with_memory_space_constraint(kv, pltpu.HBM)
    blocks = pltpu.with_memory_space_constraint(valid_blocks, pltpu.HBM)
    vmem = pl.BlockSpec(memory_space=pltpu.VMEM)
    smem = pl.BlockSpec(memory_space=pltpu.SMEM)
    anywhere = pl.BlockSpec(memory_space=pl.ANY)
    hbm = pl.BlockSpec(memory_space=pltpu.HBM)
    table = (3, kinds, user_count, width)
    dma = pltpu.SemaphoreType.DMA
    small = jax.ShapeDtypeStruct((kinds, user_count, width), jnp.float32)
    whole = jax.ShapeDtypeStruct((kinds, n * part, width), jnp.bfloat16)
    early, centers, scales, inverse, lengths, choice = pl.pallas_call(
        functools.partial(gather, n, groups, quarter),
        out_shape=(
            whole, small, small, small,
            jax.ShapeDtypeStruct((user_count, width), jnp.int32),
            jax.ShapeDtypeStruct((1,), jnp.int32),
        ),
        in_specs=[hbm, hbm],
        out_specs=(vmem,) * 5 + (smem,),
        scratch_shapes=[
            pltpu.SMEM((groups, user_count), jnp.int32),
            pltpu.VMEM((kinds, user_count, per_dev, width), jnp.bfloat16),
            pltpu.VMEM((n,) + table, jnp.float32),
            pltpu.VMEM((2,) + table, jnp.float32),
            pltpu.VMEM(table, jnp.float32),
            dma, dma, dma, dma((n, kinds)), dma((n, kinds)), dma((kinds, 2)), dma((n, kinds, 2)),
            dma, dma((n,)), dma, dma, dma((n,)), dma, dma((groups,)), dma((groups,)),
            pltpu.SemaphoreType.REGULAR,
        ],
        compiler_params=pltpu.CompilerParams(
            collective_id=0, has_side_effects=True, vmem_limit_bytes=GRANT
        ),
        name="gather",
    )(blocks, kv)

    def branch(index):
        def run(lengths, centers, inverse):
            return pl.pallas_call(
                functools.partial(remainder, index, n, groups, quarter),
                out_shape=jax.ShapeDtypeStruct((kinds, (n // 2) * part, width), jnp.bfloat16),
                in_specs=[hbm, vmem, vmem, vmem],
                out_specs=vmem,
                scratch_shapes=[
                    dma((n, kinds)), dma((kinds,)), dma((kinds,)), dma((n // 2, kinds)),
                    pltpu.SemaphoreType.REGULAR,
                ],
                compiler_params=pltpu.CompilerParams(
                    collective_id=1 + index, has_side_effects=True, vmem_limit_bytes=GRANT
                ),
                name=f"remainder_{index}",
            )(kv, lengths, centers, inverse)

        return run

    late = lax.switch(
        choice[0],
        [branch(i) for i in range(len(classes(user_count)) ** groups)],
        lengths, centers, inverse,
    )
    out, centers, scales = pl.pallas_call(
        functools.partial(finish, n, part),
        out_shape=(whole, small, small),
        in_specs=[vmem] * 4,
        out_specs=(anywhere, anywhere, anywhere),
        scratch_shapes=[dma((n + 2,))],
        compiler_params=pltpu.CompilerParams(vmem_limit_bytes=GRANT),
        name="finish",
    )(early, late, centers, scales)

    def spread(x, middle):
        x = x.reshape(kind_count, layer_dev, heads_dev, *middle, width)
        return jnp.moveaxis(x, 2, -2)

    return (
        spread(out, (1, n * part)),
        spread(centers, (user_count,)),
        spread(scales, (user_count,)),
    )


def solution(mesh):
    in_specs = (P(None, "layer", "groups", "seq", "head", None), P("groups"))
    out_specs = (
        P(None, "layer", ("groups", "seq"), None, "head", None),
        P(None, "layer", "groups", "head", None),
        P(None, "layer", "groups", "head", None),
    )
    return jax.shard_map(
        on_device, mesh=mesh, in_specs=in_specs, out_specs=out_specs, check_vma=False
    )
```

```python
import functools

import jax
import jax.numpy as jnp
from jax import lax
from jax.experimental import pallas as pl
from jax.experimental.pallas import tpu as pltpu
from jax.sharding import PartitionSpec as P

BLOCK = 128
ROWS = 8
GRANT = 16 * 2**20
EPSILON = 1e-06
CLASSES = (
    (8, 8, 8, 8),
    (6, 8, 8, 6),
    (8, 4, 8, 4),
    (8, 2, 4, 8),
    (2, 8, 2, 8),
    (8, 2, 8, 2),
    (0, 8, 8, 2),
)


def classes(users):
    return tuple(c for c in CLASSES if len(c) == users) or ((8,) * users,)


def normalised(x, first, length, center, inverse):
    x = x.astype(jnp.float32)
    position = first + lax.broadcasted_iota(jnp.int32, x.shape, 0)
    return jnp.where(position < length, (x - center) * inverse, 0.0).astype(jnp.bfloat16)


def combine(into, left, right):
    into[0] = left[0] + right[0]
    into[1] = jnp.maximum(left[1], right[1])
    into[2] = jnp.minimum(left[2], right[2])


def each(low, high, action):
    def step(i, _):
        action(i)
        return 0

    lax.fori_loop(low, high, step, 0)


def gather(n, groups, quarter, blocks_ref, kv_ref, recv_ref, centers_ref, scales_ref, inverse_ref,
           lengths_ref, choice_ref, blocks, local, stats_ref, half_ref, full_ref,
           load_sem, fetch_sem, own_sem, send_sem, recv_sem, cut_send, cut_recv, stat_send, stat_recv,
           half_send, half_recv, full_send, full_recv, swap_send, swap_recv, ready):
    kinds, users, per_dev, width = kv_ref.shape
    part = per_dev // quarter
    half = n // 2
    me = lax.axis_index("seq")
    group = lax.axis_index("groups")
    mids = (half - 1, half)
    ends = (0, n - 1)
    mid = (me == mids[0]) | (me == mids[1])
    outer = (me < mids[0]) | (me > mids[1])
    side = me // half
    partner = n - 1 - me

    load = pltpu.make_async_copy(kv_ref, local, load_sem)
    load.start()
    fetch = pltpu.make_async_copy(blocks_ref, blocks.at[group], fetch_sem)
    fetch.start()

    barrier = pltpu.get_barrier_semaphore()
    for g in range(groups):
        @pl.when(group != g)
        def _():
            pl.semaphore_signal(barrier, inc=1, device_id={"groups": g})
    for d in range(n):
        greets = (mid if d in mids else me >= 0) & (me != d)

        @pl.when(greets)
        def _():
            pl.semaphore_signal(barrier, inc=1, device_id={"seq": d})

    @pl.when(mid)
    def _():
        pl.semaphore_wait(barrier, groups)

    @pl.when(outer)
    def _():
        pl.semaphore_wait(barrier, n + groups - 2)
        for d in mids:
            pl.semaphore_signal(ready, inc=1, device_id={"seq": d})

    def bulk(source, target, k):
        user, q = target // quarter, target % quarter
        return pltpu.make_async_remote_copy(
            src_ref=local.at[k, user, pl.ds(pl.multiple_of(q * part, part), part), :],
            dst_ref=recv_ref.at[k, pl.ds(pl.multiple_of(source * part, part), part), :],
            send_sem=send_sem.at[target, k],
            recv_sem=recv_sem.at[source, k],
            device_id={"seq": target},
        )

    def cut(source, target, k, i, src=local):
        user, q = target // quarter, target % quarter
        rows = part // 2
        return pltpu.make_async_remote_copy(
            src_ref=src.at[k, user, pl.ds(pl.multiple_of(q * part + i * rows, rows), rows), :],
            dst_ref=recv_ref.at[k, pl.ds(pl.multiple_of(source * part + i * rows, rows), rows), :],
            send_sem=cut_send.at[k, i],
            recv_sem=cut_recv.at[source, k, i],
            device_id={"seq": target},
        )

    def stat(source, target):
        return pltpu.make_async_remote_copy(
            src_ref=stats_ref.at[source],
            dst_ref=stats_ref.at[source],
            send_sem=stat_send,
            recv_sem=stat_recv.at[source],
            device_id={"seq": target},
        )

    def across(origin):
        return pltpu.make_async_remote_copy(
            src_ref=half_ref.at[origin],
            dst_ref=half_ref.at[origin],
            send_sem=half_send,
            recv_sem=half_recv,
            device_id={"seq": partner},
        )

    def handed(target):
        return pltpu.make_async_remote_copy(
            src_ref=full_ref,
            dst_ref=full_ref,
            send_sem=full_send.at[target],
            recv_sem=full_recv,
            device_id={"seq": target},
        )

    def swap(origin, g):
        return pltpu.make_async_remote_copy(
            src_ref=blocks.at[origin],
            dst_ref=blocks.at[origin],
            send_sem=swap_send.at[g],
            recv_sem=swap_recv.at[origin],
            device_id={"groups": g},
        )

    @pl.when(outer)
    def _():
        load.wait()

    for h in range(2):
        @pl.when(outer & (side == h))
        def _():
            cut(me, mids[1 - h], 0, 0, kv_ref).start()

    own = pltpu.make_async_copy(
        kv_ref.at[:, me // quarter, pl.ds(pl.multiple_of((me % quarter) * part, part), part), :],
        recv_ref.at[:, pl.ds(pl.multiple_of(me * part, part), part), :],
        own_sem,
    )
    own.start()
    fetch.wait()
    for g in range(groups):
        @pl.when(group != g)
        def _():
            swap(group, g).start()

    @pl.when(mid)
    def _():
        load.wait()

    for u in range(users):
        lengths_ref[pl.ds(u, 1), :] = jnp.full((1, width), blocks[group, u] * BLOCK, jnp.int32)
    count = per_dev // BLOCK
    for k in range(kinds):
        for u in range(users):
            live = blocks[group, u] - me * count

            def step(b, carry, k=k, u=u, live=live):
                total, high, low = carry
                x = local[k, u, pl.ds(pl.multiple_of(b * BLOCK, BLOCK), BLOCK), :].astype(jnp.float32)
                x = x.reshape(BLOCK // ROWS, ROWS, width)
                on = b < live
                total = total + jnp.where(on, jnp.sum(x, axis=0), 0.0)
                high = jnp.maximum(high, jnp.where(on, jnp.max(x, axis=0), -jnp.inf))
                low = jnp.minimum(low, jnp.where(on, jnp.min(x, axis=0), jnp.inf))
                return total, high, low

            shape = (ROWS, width)
            total, high, low = lax.fori_loop(
                0, count, step,
                (jnp.zeros(shape, jnp.float32), jnp.full(shape, -jnp.inf, jnp.float32),
                 jnp.full(shape, jnp.inf, jnp.float32)),
            )
            stats_ref[me, 0, k, u, :] = jnp.sum(total, axis=0)
            stats_ref[me, 1, k, u, :] = jnp.max(high, axis=0)
            stats_ref[me, 2, k, u, :] = jnp.min(low, axis=0)

    if n > 2:
        @pl.when(mid)
        def _():
            pl.semaphore_wait(ready, n - 2)

    odd = lax.axis_index("layer") % 2 == 1

    for h in range(2):
        halves = range(h * half, (h + 1) * half)
        others = [s for s in halves if s != ends[h]]
        there = [s for s in range(n) if s // half != h and s not in mids]

        @pl.when((side == h) & (me != ends[h]))
        def _():
            stat(me, ends[h]).start()

        @pl.when(outer & (me != ends[h]) & (side == h))
        def _():
            for k in range(kinds):
                for i in range(2):
                    if k + i:
                        cut(me, mids[1 - h], k, i).start()

        @pl.when(me == ends[h])
        def _():
            @pl.when(odd)
            def _():
                cut(me, mids[1 - h], 0, 1).start()

            half_ref[h] = stats_ref[ends[h]]
            for s in others:
                stat(s, me).wait_recv()
                combine(half_ref.at[h], half_ref.at[h], stats_ref.at[s])
            across(h).start()

            @pl.when(~odd)
            def _():
                cut(me, mids[1 - h], 0, 1).start()

            for k in range(1, kinds):
                cut(me, mids[1 - h], k, 0).start()

            @pl.when(odd)
            def _():
                for k in range(1, kinds):
                    cut(me, mids[1 - h], k, 1).start()

            across(1 - h).wait_recv()
            combine(full_ref, half_ref.at[0], half_ref.at[1])
            for s in others:
                handed(s).start()

            @pl.when(~odd)
            def _():
                for k in range(1, kinds):
                    cut(me, mids[1 - h], k, 1).start()

        for s in halves:
            @pl.when(me == s)
            def _():
                targets = (there if s not in mids else []) + [t for t in halves if t != s and t not in mids]
                for t in targets:
                    for k in range(kinds):
                        bulk(me, t, k).start()

    for g in range(groups):
        @pl.when(group != g)
        def _():
            swap(g, g).wait_recv()
    options = classes(users)
    choice = jnp.int32(0)
    for g in range(groups):
        pick = jnp.int32(0)
        for c, caps in enumerate(options):
            covers = None
            for u in range(users):
                source = mids[0] if u * quarter >= half else mids[1]
                most = source * per_dev + caps[u] * per_dev // 8
                fits = (blocks[g, u] * BLOCK <= most) if caps[u] < 8 else None
                if fits is not None:
                    covers = fits if covers is None else covers & fits
            pick = jnp.int32(c) if covers is None else jnp.where(covers, c, pick)
        choice = choice * len(options) + pick
    choice_ref[0] = choice

    @pl.when((me != ends[0]) & (me != ends[1]))
    def _():
        handed(me).wait_recv()

    for u in range(users):
        length = lengths_ref[u, :].astype(jnp.float32)
        for k in range(kinds):
            total, high, low = full_ref[0, k, u, :], full_ref[1, k, u, :], full_ref[2, k, u, :]
            center = total / length
            scale = jnp.maximum(high - center, center - low) + EPSILON
            centers_ref[k, u, :] = center
            scales_ref[k, u, :] = scale
            inverse_ref[k, u, :] = 1.0 / scale

    user = me // quarter
    base = (me % quarter) * part
    length = lengths_ref[pl.ds(user, 1), :]

    def normalise(source, k, rows):
        center = centers_ref[k, pl.ds(user, 1), :]
        inverse = inverse_ref[k, pl.ds(user, 1), :]
        step = part // 4

        def at(i):
            place = pl.ds(pl.multiple_of(source * part + i * step, step), step)
            first = source * per_dev + base + i * step
            recv_ref[k, place, :] = normalised(recv_ref[k, place, :], first, length, center, inverse)

        each(0, rows // step, at)

    own.wait()
    each(0, kinds, lambda k: normalise(me, k, part))

    def arrive(source):
        def at(k):
            bulk(source, me, k).wait_recv()
            normalise(source, k, part)

        each(0, kinds, at)

    for h in range(2):
        halves = range(h * half, (h + 1) * half)
        there = [s for s in range(n) if s // half != h and s not in mids]

        @pl.when(side == h)
        def _():
            @pl.when(outer)
            def _():
                for s in halves:
                    @pl.when(me != s)
                    def _():
                        arrive(s)

            for s in there:
                @pl.when(outer)
                def _():
                    arrive(s)

                @pl.when(mid)
                def _():
                    def at(k):
                        for i in range(2):
                            cut(s, me, k, i).wait_recv()
                        normalise(s, k, part)

                    each(0, kinds, at)

            for t in halves:
                if t not in mids:
                    @pl.when(me != t)
                    def _():
                        for k in range(kinds):
                            bulk(me, t, k).wait_send()

            @pl.when(outer)
            def _():
                for t in there:
                    for k in range(kinds):
                        bulk(me, t, k).wait_send()
                for k in range(kinds):
                    for i in range(2):
                        cut(me, mids[1 - h], k, i).wait_send()

            @pl.when(me != ends[h])
            def _():
                stat(me, ends[h]).wait_send()

            @pl.when(me == ends[h])
            def _():
                across(h).wait_send()
                for s in halves:
                    if s != ends[h]:
                        handed(s).wait_send()

    for g in range(groups):
        @pl.when(group != g)
        def _():
            swap(group, g).wait_send()


def remainder(index, n, groups, quarter, kv_ref, lengths_ref, centers_ref, inverse_ref, recv_ref,
              send_sem, recv_sem, near_send, near_recv, ready):
    kinds, users, per_dev, width = kv_ref.shape
    part = per_dev // quarter
    half = n // 2
    options = classes(users)
    me = lax.axis_index("seq")
    group = lax.axis_index("groups")
    mids = (half - 1, half)
    mid = (me == mids[0]) | (me == mids[1])
    outer = (me < mids[0]) | (me > mids[1])
    side = me // half

    barrier = pltpu.get_barrier_semaphore()
    for d in range(n):
        @pl.when(mid & (me != d))
        def _():
            pl.semaphore_signal(barrier, inc=1, device_id={"seq": d})

    @pl.when(mid)
    def _():
        pl.semaphore_wait(barrier, 1)

    @pl.when(outer)
    def _():
        pl.semaphore_wait(barrier, 2)
        for d in mids:
            pl.semaphore_signal(ready, inc=1, device_id={"seq": d})

    def window(target, caps):
        rows = caps[target // quarter] * per_dev // 8 - (target % quarter) * part
        return max(min(rows, part), 0)

    def late(target, caps, k):
        rows = window(target, caps)
        user, q = target // quarter, target % quarter
        return pltpu.make_async_remote_copy(
            src_ref=kv_ref.at[k, user, pl.ds(q * part, rows), :],
            dst_ref=recv_ref.at[k, pl.ds(0, rows), :],
            send_sem=send_sem.at[target, k],
            recv_sem=recv_sem.at[k],
            device_id={"seq": target},
        )

    def near(source, h, k):
        target = mids[h]
        user, q = target // quarter, target % quarter
        slot = 1 + (source if h == 0 else n - 1 - source)
        return pltpu.make_async_remote_copy(
            src_ref=kv_ref.at[k, user, pl.ds(q * part, part), :],
            dst_ref=recv_ref.at[k, pl.ds(slot * part, part), :],
            send_sem=near_send.at[k],
            recv_sem=near_recv.at[slot, k],
            device_id={"seq": target},
        )

    picks = []
    for g in reversed(range(groups)):
        picks.insert(0, options[index // len(options) ** (groups - 1 - g) % len(options)])

    def both(action):
        for g in range(groups):
            @pl.when(group == g)
            def _():
                action(picks[g])

    for h in range(2):
        for s in range(h * half, (h + 1) * half):
            if s not in mids:
                @pl.when(me == s)
                def _():
                    for k in range(kinds):
                        near(s, h, k).start()

    def split(h, caps):
        return kinds if 2 * window(mids[1 - h], caps) <= part else 1

    def send(targets, caps, which):
        for t in targets:
            for k in which:
                if window(t, caps):
                    late(t, caps, k).start()

    for h in range(2):
        away = [t for t in range(n) if t // half != h and t not in mids]

        @pl.when(me == mids[h])
        def _():
            both(lambda caps: send([mids[1 - h]], caps, range(split(h, caps))))
            if n > 2:
                pl.semaphore_wait(ready, n - 2)
            both(lambda caps: (
                send(away, caps, range(kinds)),
                send([mids[1 - h]], caps, range(split(h, caps), kinds)),
            ))

    user = me // quarter
    base = (me % quarter) * part
    length = lengths_ref[pl.ds(user, 1), :]
    step = part // 8

    def put(slot, source, k, i):
        center = centers_ref[k, pl.ds(user, 1), :]
        inverse = inverse_ref[k, pl.ds(user, 1), :]
        place = pl.ds(pl.multiple_of(slot * part + i * step, step), step)
        first = source * per_dev + base + i * step
        recv_ref[k, place, :] = normalised(recv_ref[k, place, :], first, length, center, inverse)

    def clear(k, i):
        recv_ref[k, pl.ds(pl.multiple_of(i * step, step), step), :] = jnp.zeros((step, width), jnp.bfloat16)

    for h in range(2):
        @pl.when(mid & (side == h))
        def _():
            for s in range(h * half, (h + 1) * half):
                if s not in mids:
                    slot = 1 + (s if h == 0 else n - 1 - s)
                    for k in range(kinds):
                        near(s, h, k).wait_recv()
                    each(0, kinds, lambda k: each(0, part // step, lambda i: put(slot, s, k, i)))

    for k in range(kinds):
        high = jnp.int32(0)
        for t in range(n):
            for g in range(groups):
                rows = window(t, picks[g])
                here = (me == t) & (group == g)
                high = jnp.where(here, rows // step, high)
                if rows:
                    @pl.when(here)
                    def _():
                        late(t, picks[g], k).wait_recv()
        each(0, high, lambda i: put(0, mids[0] + 1 - side, k, i))
        each(high, part // step, lambda i: clear(k, i))

    def drain(targets, caps):
        for t in targets:
            for k in range(kinds):
                if window(t, caps):
                    late(t, caps, k).wait_send()

    for h in range(2):
        away = [t for t in range(n) if t // half != h]

        @pl.when(me == mids[h])
        def _():
            both(lambda caps: drain(away, caps))

        for s in range(h * half, (h + 1) * half):
            if s not in mids:
                @pl.when(me == s)
                def _():
                    for k in range(kinds):
                        near(s, h, k).wait_send()


def finish(n, part, early_ref, late_ref, c_ref, s_ref, out_ref, centers_ref, scales_ref, sems):
    half = n // 2
    mids = (half - 1, half)
    me = lax.axis_index("seq")
    for t in range(n):
        @pl.when(me == t)
        def _():
            h = t // half
            pieces = []
            for s in range(n):
                at = s * part
                if s == mids[1 - h]:
                    pieces.append((late_ref, 0, at, part))
                elif t in mids and s != t and s // half == h:
                    pieces.append((late_ref, (1 + (s if h == 0 else n - 1 - s)) * part, at, part))
                elif pieces and pieces[-1][0] is early_ref:
                    _, a, b, rows = pieces.pop()
                    pieces.append((early_ref, a, b, rows + part))
                else:
                    pieces.append((early_ref, at, at, part))
            copies = [
                pltpu.make_async_copy(
                    ref.at[:, pl.ds(a, rows), :], out_ref.at[:, pl.ds(b, rows), :], sems.at[i])
                for i, (ref, a, b, rows) in enumerate(pieces)
            ] + [
                pltpu.make_async_copy(c_ref, centers_ref, sems.at[n]),
                pltpu.make_async_copy(s_ref, scales_ref, sems.at[n + 1]),
            ]
            for copy in copies:
                copy.start()
            for copy in copies:
                copy.wait()


def on_device(kv_cache, valid_blocks):
    kind_count, layer_dev, user_count, per_dev, heads_dev, width = kv_cache.shape
    n, groups = lax.axis_size("seq"), lax.axis_size("groups")
    quarter = n // user_count
    part = per_dev // quarter
    kinds = kind_count * layer_dev * heads_dev
    kv = jnp.transpose(kv_cache, (0, 1, 4, 2, 3, 5)).reshape(kinds, user_count, per_dev, width)
    kv = pltpu.with_memory_space_constraint(kv, pltpu.HBM)
    blocks = pltpu.with_memory_space_constraint(valid_blocks, pltpu.HBM)
    vmem = pl.BlockSpec(memory_space=pltpu.VMEM)
    smem = pl.BlockSpec(memory_space=pltpu.SMEM)
    anywhere = pl.BlockSpec(memory_space=pl.ANY)
    hbm = pl.BlockSpec(memory_space=pltpu.HBM)
    table = (3, kinds, user_count, width)
    dma = pltpu.SemaphoreType.DMA
    small = jax.ShapeDtypeStruct((kinds, user_count, width), jnp.float32)
    whole = jax.ShapeDtypeStruct((kinds, n * part, width), jnp.bfloat16)
    early, centers, scales, inverse, lengths, choice = pl.pallas_call(
        functools.partial(gather, n, groups, quarter),
        out_shape=(
            whole, small, small, small,
            jax.ShapeDtypeStruct((user_count, width), jnp.int32),
            jax.ShapeDtypeStruct((1,), jnp.int32),
        ),
        in_specs=[hbm, hbm],
        out_specs=(vmem,) * 5 + (smem,),
        scratch_shapes=[
            pltpu.SMEM((groups, user_count), jnp.int32),
            pltpu.VMEM((kinds, user_count, per_dev, width), jnp.bfloat16),
            pltpu.VMEM((n,) + table, jnp.float32),
            pltpu.VMEM((2,) + table, jnp.float32),
            pltpu.VMEM(table, jnp.float32),
            dma, dma, dma, dma((n, kinds)), dma((n, kinds)), dma((kinds, 2)), dma((n, kinds, 2)),
            dma, dma((n,)), dma, dma, dma((n,)), dma, dma((groups,)), dma((groups,)),
            pltpu.SemaphoreType.REGULAR,
        ],
        compiler_params=pltpu.CompilerParams(
            collective_id=0, has_side_effects=True, vmem_limit_bytes=GRANT
        ),
        name="gather",
    )(blocks, kv)

    def branch(index):
        def run(lengths, centers, inverse):
            return pl.pallas_call(
                functools.partial(remainder, index, n, groups, quarter),
                out_shape=jax.ShapeDtypeStruct((kinds, (n // 2) * part, width), jnp.bfloat16),
                in_specs=[hbm, vmem, vmem, vmem],
                out_specs=vmem,
                scratch_shapes=[
                    dma((n, kinds)), dma((kinds,)), dma((kinds,)), dma((n // 2, kinds)),
                    pltpu.SemaphoreType.REGULAR,
                ],
                compiler_params=pltpu.CompilerParams(
                    collective_id=1 + index, has_side_effects=True, vmem_limit_bytes=GRANT
                ),
                name=f"remainder_{index}",
            )(kv, lengths, centers, inverse)

        return run

    late = lax.switch(
        choice[0],
        [branch(i) for i in range(len(classes(user_count)) ** groups)],
        lengths, centers, inverse,
    )
    out, centers, scales = pl.pallas_call(
        functools.partial(finish, n, part),
        out_shape=(whole, small, small),
        in_specs=[vmem] * 4,
        out_specs=(anywhere, anywhere, anywhere),
        scratch_shapes=[dma((n + 2,))],
        compiler_params=pltpu.CompilerParams(vmem_limit_bytes=GRANT),
        name="finish",
    )(early, late, centers, scales)

    def spread(x, middle):
        x = x.reshape(kind_count, layer_dev, heads_dev, *middle, width)
        return jnp.moveaxis(x, 2, -2)

    return (
        spread(out, (1, n * part)),
        spread(centers, (user_count,)),
        spread(scales, (user_count,)),
    )


def solution(mesh):
    in_specs = (P(None, "layer", "groups", "seq", "head", None), P("groups"))
    out_specs = (
        P(None, "layer", ("groups", "seq"), None, "head", None),
        P(None, "layer", "groups", "head", None),
        P(None, "layer", "groups", "head", None),
    )
    return jax.shard_map(
        on_device, mesh=mesh, in_specs=in_specs, out_specs=out_specs, check_vma=False
    )
```

```python
import functools

import jax
import jax.numpy as jnp
from jax import lax
from jax.experimental import pallas as pl
from jax.experimental.pallas import tpu as pltpu
from jax.sharding import PartitionSpec as P

BLOCK = 128
ROWS = 8
GRANT = 16 * 2**20
EPSILON = 1e-06
CLASSES = (
    (8, 8, 8, 8),
    (8, 6, 6, 8),
    (6, 8, 8, 6),
    (8, 4, 8, 4),
    (8, 2, 4, 8),
    (2, 8, 2, 8),
    (8, 2, 8, 2),
    (0, 8, 8, 2),
)


def classes(users):
    return tuple(c for c in CLASSES if len(c) == users) or ((8,) * users,)


def normalised(x, first, length, center, inverse):
    x = x.astype(jnp.float32)
    position = first + lax.broadcasted_iota(jnp.int32, x.shape, 0)
    return jnp.where(position < length, (x - center) * inverse, 0.0).astype(jnp.bfloat16)


def combine(into, left, right):
    into[0] = left[0] + right[0]
    into[1] = jnp.maximum(left[1], right[1])
    into[2] = jnp.minimum(left[2], right[2])


def each(low, high, action):
    def step(i, _):
        action(i)
        return 0

    lax.fori_loop(low, high, step, 0)


def gather(n, groups, quarter, blocks_ref, kv_ref, recv_ref, centers_ref, scales_ref, inverse_ref,
           lengths_ref, choice_ref, blocks, local, stats_ref, half_ref, full_ref,
           load_sem, fetch_sem, own_sem, send_sem, recv_sem, cut_send, cut_recv, stat_send, stat_recv,
           half_send, half_recv, full_send, full_recv, swap_send, swap_recv, ready):
    kinds, users, per_dev, width = kv_ref.shape
    part = per_dev // quarter
    half = n // 2
    me = lax.axis_index("seq")
    group = lax.axis_index("groups")
    mids = (half - 1, half)
    ends = (0, n - 1)
    mid = (me == mids[0]) | (me == mids[1])
    outer = (me < mids[0]) | (me > mids[1])
    side = me // half
    partner = n - 1 - me

    load = pltpu.make_async_copy(kv_ref, local, load_sem)
    load.start()
    fetch = pltpu.make_async_copy(blocks_ref, blocks.at[group], fetch_sem)
    fetch.start()

    barrier = pltpu.get_barrier_semaphore()
    for g in range(groups):
        @pl.when(group != g)
        def _():
            pl.semaphore_signal(barrier, inc=1, device_id={"groups": g})
    for d in range(n):
        greets = (mid if d in mids else me >= 0) & (me != d)

        @pl.when(greets)
        def _():
            pl.semaphore_signal(barrier, inc=1, device_id={"seq": d})

    @pl.when(mid)
    def _():
        pl.semaphore_wait(barrier, groups)

    @pl.when(outer)
    def _():
        pl.semaphore_wait(barrier, n + groups - 2)
        for d in mids:
            pl.semaphore_signal(ready, inc=1, device_id={"seq": d})

    def bulk(source, target, k):
        user, q = target // quarter, target % quarter
        return pltpu.make_async_remote_copy(
            src_ref=local.at[k, user, pl.ds(pl.multiple_of(q * part, part), part), :],
            dst_ref=recv_ref.at[k, pl.ds(pl.multiple_of(source * part, part), part), :],
            send_sem=send_sem.at[target, k],
            recv_sem=recv_sem.at[source, k],
            device_id={"seq": target},
        )

    def cut(source, target, k, i, src=local):
        user, q = target // quarter, target % quarter
        rows = part // 2
        return pltpu.make_async_remote_copy(
            src_ref=src.at[k, user, pl.ds(pl.multiple_of(q * part + i * rows, rows), rows), :],
            dst_ref=recv_ref.at[k, pl.ds(pl.multiple_of(source * part + i * rows, rows), rows), :],
            send_sem=cut_send.at[k, i],
            recv_sem=cut_recv.at[source, k, i],
            device_id={"seq": target},
        )

    def stat(source, target):
        return pltpu.make_async_remote_copy(
            src_ref=stats_ref.at[source],
            dst_ref=stats_ref.at[source],
            send_sem=stat_send,
            recv_sem=stat_recv.at[source],
            device_id={"seq": target},
        )

    def across(origin):
        return pltpu.make_async_remote_copy(
            src_ref=half_ref.at[origin],
            dst_ref=half_ref.at[origin],
            send_sem=half_send,
            recv_sem=half_recv,
            device_id={"seq": partner},
        )

    def handed(target):
        return pltpu.make_async_remote_copy(
            src_ref=full_ref,
            dst_ref=full_ref,
            send_sem=full_send.at[target],
            recv_sem=full_recv,
            device_id={"seq": target},
        )

    def swap(origin, g):
        return pltpu.make_async_remote_copy(
            src_ref=blocks.at[origin],
            dst_ref=blocks.at[origin],
            send_sem=swap_send.at[g],
            recv_sem=swap_recv.at[origin],
            device_id={"groups": g},
        )

    @pl.when(outer)
    def _():
        load.wait()

    for h in range(2):
        @pl.when(outer & (side == h))
        def _():
            cut(me, mids[1 - h], 0, 0, kv_ref).start()

    own = pltpu.make_async_copy(
        kv_ref.at[:, me // quarter, pl.ds(pl.multiple_of((me % quarter) * part, part), part), :],
        recv_ref.at[:, pl.ds(pl.multiple_of(me * part, part), part), :],
        own_sem,
    )
    own.start()
    fetch.wait()
    for g in range(groups):
        @pl.when(group != g)
        def _():
            swap(group, g).start()

    @pl.when(mid)
    def _():
        load.wait()

    for u in range(users):
        lengths_ref[pl.ds(u, 1), :] = jnp.full((1, width), blocks[group, u] * BLOCK, jnp.int32)
    count = per_dev // BLOCK
    for k in range(kinds):
        for u in range(users):
            live = blocks[group, u] - me * count

            def step(b, carry, k=k, u=u, live=live):
                total, high, low = carry
                x = local[k, u, pl.ds(pl.multiple_of(b * BLOCK, BLOCK), BLOCK), :].astype(jnp.float32)
                x = x.reshape(BLOCK // ROWS, ROWS, width)
                on = b < live
                total = total + jnp.where(on, jnp.sum(x, axis=0), 0.0)
                high = jnp.maximum(high, jnp.where(on, jnp.max(x, axis=0), -jnp.inf))
                low = jnp.minimum(low, jnp.where(on, jnp.min(x, axis=0), jnp.inf))
                return total, high, low

            shape = (ROWS, width)
            total, high, low = lax.fori_loop(
                0, count, step,
                (jnp.zeros(shape, jnp.float32), jnp.full(shape, -jnp.inf, jnp.float32),
                 jnp.full(shape, jnp.inf, jnp.float32)),
            )
            stats_ref[me, 0, k, u, :] = jnp.sum(total, axis=0)
            stats_ref[me, 1, k, u, :] = jnp.max(high, axis=0)
            stats_ref[me, 2, k, u, :] = jnp.min(low, axis=0)

    if n > 2:
        @pl.when(mid)
        def _():
            pl.semaphore_wait(ready, n - 2)

    odd = lax.axis_index("layer") % 2 == 1

    for h in range(2):
        halves = range(h * half, (h + 1) * half)
        others = [s for s in halves if s != ends[h]]
        there = [s for s in range(n) if s // half != h and s not in mids]

        @pl.when((side == h) & (me != ends[h]))
        def _():
            stat(me, ends[h]).start()

        @pl.when(outer & (me != ends[h]) & (side == h))
        def _():
            for k in range(kinds):
                for i in range(2):
                    if k + i:
                        cut(me, mids[1 - h], k, i).start()

        @pl.when(me == ends[h])
        def _():
            @pl.when(odd)
            def _():
                cut(me, mids[1 - h], 0, 1).start()

            half_ref[h] = stats_ref[ends[h]]
            for s in others:
                stat(s, me).wait_recv()
                combine(half_ref.at[h], half_ref.at[h], stats_ref.at[s])
            across(h).start()

            @pl.when(~odd)
            def _():
                cut(me, mids[1 - h], 0, 1).start()

            for k in range(1, kinds):
                cut(me, mids[1 - h], k, 0).start()

            @pl.when(odd)
            def _():
                for k in range(1, kinds):
                    cut(me, mids[1 - h], k, 1).start()

            across(1 - h).wait_recv()
            combine(full_ref, half_ref.at[0], half_ref.at[1])
            for s in others:
                handed(s).start()

            @pl.when(~odd)
            def _():
                for k in range(1, kinds):
                    cut(me, mids[1 - h], k, 1).start()

        for s in halves:
            @pl.when(me == s)
            def _():
                targets = (there if s not in mids else []) + [t for t in halves if t != s and t not in mids]
                for t in targets:
                    for k in range(kinds):
                        bulk(me, t, k).start()

    for g in range(groups):
        @pl.when(group != g)
        def _():
            swap(g, g).wait_recv()
    options = classes(users)
    choice = jnp.int32(0)
    for g in range(groups):
        pick = jnp.int32(0)
        for c, caps in enumerate(options):
            covers = None
            for u in range(users):
                source = mids[0] if u * quarter >= half else mids[1]
                most = source * per_dev + caps[u] * per_dev // 8
                fits = (blocks[g, u] * BLOCK <= most) if caps[u] < 8 else None
                if fits is not None:
                    covers = fits if covers is None else covers & fits
            pick = jnp.int32(c) if covers is None else jnp.where(covers, c, pick)
        choice = choice * len(options) + pick
    choice_ref[0] = choice

    @pl.when((me != ends[0]) & (me != ends[1]))
    def _():
        handed(me).wait_recv()

    for u in range(users):
        length = lengths_ref[u, :].astype(jnp.float32)
        for k in range(kinds):
            total, high, low = full_ref[0, k, u, :], full_ref[1, k, u, :], full_ref[2, k, u, :]
            center = total / length
            scale = jnp.maximum(high - center, center - low) + EPSILON
            centers_ref[k, u, :] = center
            scales_ref[k, u, :] = scale
            inverse_ref[k, u, :] = 1.0 / scale

    user = me // quarter
    base = (me % quarter) * part
    length = lengths_ref[pl.ds(user, 1), :]

    def normalise(source, k, rows):
        center = centers_ref[k, pl.ds(user, 1), :]
        inverse = inverse_ref[k, pl.ds(user, 1), :]
        step = part // 4

        def at(i):
            place = pl.ds(pl.multiple_of(source * part + i * step, step), step)
            first = source * per_dev + base + i * step
            recv_ref[k, place, :] = normalised(recv_ref[k, place, :], first, length, center, inverse)

        each(0, rows // step, at)

    own.wait()
    each(0, kinds, lambda k: normalise(me, k, part))

    def arrive(source):
        def at(k):
            bulk(source, me, k).wait_recv()
            normalise(source, k, part)

        each(0, kinds, at)

    for h in range(2):
        halves = range(h * half, (h + 1) * half)
        there = [s for s in range(n) if s // half != h and s not in mids]

        @pl.when(side == h)
        def _():
            @pl.when(outer)
            def _():
                for s in halves:
                    @pl.when(me != s)
                    def _():
                        arrive(s)

            for s in there:
                @pl.when(outer)
                def _():
                    arrive(s)

                @pl.when(mid)
                def _():
                    def at(k):
                        for i in range(2):
                            cut(s, me, k, i).wait_recv()
                        normalise(s, k, part)

                    each(0, kinds, at)

            for t in halves:
                if t not in mids:
                    @pl.when(me != t)
                    def _():
                        for k in range(kinds):
                            bulk(me, t, k).wait_send()

            @pl.when(outer)
            def _():
                for t in there:
                    for k in range(kinds):
                        bulk(me, t, k).wait_send()
                for k in range(kinds):
                    for i in range(2):
                        cut(me, mids[1 - h], k, i).wait_send()

            @pl.when(me != ends[h])
            def _():
                stat(me, ends[h]).wait_send()

            @pl.when(me == ends[h])
            def _():
                across(h).wait_send()
                for s in halves:
                    if s != ends[h]:
                        handed(s).wait_send()

    for g in range(groups):
        @pl.when(group != g)
        def _():
            swap(group, g).wait_send()


def remainder(index, n, groups, quarter, kv_ref, lengths_ref, centers_ref, inverse_ref, recv_ref,
              send_sem, recv_sem, near_send, near_recv, ready):
    kinds, users, per_dev, width = kv_ref.shape
    part = per_dev // quarter
    half = n // 2
    options = classes(users)
    me = lax.axis_index("seq")
    group = lax.axis_index("groups")
    mids = (half - 1, half)
    mid = (me == mids[0]) | (me == mids[1])
    outer = (me < mids[0]) | (me > mids[1])
    side = me // half

    barrier = pltpu.get_barrier_semaphore()
    for d in range(n):
        @pl.when(mid & (me != d))
        def _():
            pl.semaphore_signal(barrier, inc=1, device_id={"seq": d})

    @pl.when(mid)
    def _():
        pl.semaphore_wait(barrier, 1)

    @pl.when(outer)
    def _():
        pl.semaphore_wait(barrier, 2)
        for d in mids:
            pl.semaphore_signal(ready, inc=1, device_id={"seq": d})

    def window(target, caps):
        rows = caps[target // quarter] * per_dev // 8 - (target % quarter) * part
        return max(min(rows, part), 0)

    def late(target, caps, k):
        rows = window(target, caps)
        user, q = target // quarter, target % quarter
        return pltpu.make_async_remote_copy(
            src_ref=kv_ref.at[k, user, pl.ds(q * part, rows), :],
            dst_ref=recv_ref.at[k, pl.ds(0, rows), :],
            send_sem=send_sem.at[target, k],
            recv_sem=recv_sem.at[k],
            device_id={"seq": target},
        )

    def near(source, h, k):
        target = mids[h]
        user, q = target // quarter, target % quarter
        slot = 1 + (source if h == 0 else n - 1 - source)
        return pltpu.make_async_remote_copy(
            src_ref=kv_ref.at[k, user, pl.ds(q * part, part), :],
            dst_ref=recv_ref.at[k, pl.ds(slot * part, part), :],
            send_sem=near_send.at[k],
            recv_sem=near_recv.at[slot, k],
            device_id={"seq": target},
        )

    picks = []
    for g in reversed(range(groups)):
        picks.insert(0, options[index // len(options) ** (groups - 1 - g) % len(options)])

    def both(action):
        for g in range(groups):
            @pl.when(group == g)
            def _():
                action(picks[g])

    for h in range(2):
        for s in range(h * half, (h + 1) * half):
            if s not in mids:
                @pl.when(me == s)
                def _():
                    for k in range(kinds):
                        near(s, h, k).start()

    def split(h, caps):
        return kinds if 2 * window(mids[1 - h], caps) <= part else 1

    def send(targets, caps, which):
        for t in targets:
            for k in which:
                if window(t, caps):
                    late(t, caps, k).start()

    for h in range(2):
        away = [t for t in range(n) if t // half != h and t not in mids]

        @pl.when(me == mids[h])
        def _():
            both(lambda caps: send([mids[1 - h]], caps, range(split(h, caps))))
            if n > 2:
                pl.semaphore_wait(ready, n - 2)
            both(lambda caps: (
                send(away, caps, range(kinds)),
                send([mids[1 - h]], caps, range(split(h, caps), kinds)),
            ))

    user = me // quarter
    base = (me % quarter) * part
    length = lengths_ref[pl.ds(user, 1), :]
    step = part // 8

    def put(slot, source, k, i):
        center = centers_ref[k, pl.ds(user, 1), :]
        inverse = inverse_ref[k, pl.ds(user, 1), :]
        place = pl.ds(pl.multiple_of(slot * part + i * step, step), step)
        first = source * per_dev + base + i * step
        recv_ref[k, place, :] = normalised(recv_ref[k, place, :], first, length, center, inverse)

    def clear(k, i):
        recv_ref[k, pl.ds(pl.multiple_of(i * step, step), step), :] = jnp.zeros((step, width), jnp.bfloat16)

    for h in range(2):
        @pl.when(mid & (side == h))
        def _():
            for s in range(h * half, (h + 1) * half):
                if s not in mids:
                    slot = 1 + (s if h == 0 else n - 1 - s)
                    for k in range(kinds):
                        near(s, h, k).wait_recv()
                    each(0, kinds, lambda k: each(0, part // step, lambda i: put(slot, s, k, i)))

    for k in range(kinds):
        high = jnp.int32(0)
        for t in range(n):
            for g in range(groups):
                rows = window(t, picks[g])
                here = (me == t) & (group == g)
                high = jnp.where(here, rows // step, high)
                if rows:
                    @pl.when(here)
                    def _():
                        late(t, picks[g], k).wait_recv()
        each(0, high, lambda i: put(0, mids[0] + 1 - side, k, i))
        each(high, part // step, lambda i: clear(k, i))

    def drain(targets, caps):
        for t in targets:
            for k in range(kinds):
                if window(t, caps):
                    late(t, caps, k).wait_send()

    for h in range(2):
        away = [t for t in range(n) if t // half != h]

        @pl.when(me == mids[h])
        def _():
            both(lambda caps: drain(away, caps))

        for s in range(h * half, (h + 1) * half):
            if s not in mids:
                @pl.when(me == s)
                def _():
                    for k in range(kinds):
                        near(s, h, k).wait_send()


def finish(n, part, early_ref, late_ref, c_ref, s_ref, out_ref, centers_ref, scales_ref, sems):
    half = n // 2
    mids = (half - 1, half)
    me = lax.axis_index("seq")
    for t in range(n):
        @pl.when(me == t)
        def _():
            h = t // half
            pieces = []
            for s in range(n):
                at = s * part
                if s == mids[1 - h]:
                    pieces.append((late_ref, 0, at, part))
                elif t in mids and s != t and s // half == h:
                    pieces.append((late_ref, (1 + (s if h == 0 else n - 1 - s)) * part, at, part))
                elif pieces and pieces[-1][0] is early_ref:
                    _, a, b, rows = pieces.pop()
                    pieces.append((early_ref, a, b, rows + part))
                else:
                    pieces.append((early_ref, at, at, part))
            copies = [
                pltpu.make_async_copy(
                    ref.at[:, pl.ds(a, rows), :], out_ref.at[:, pl.ds(b, rows), :], sems.at[i])
                for i, (ref, a, b, rows) in enumerate(pieces)
            ] + [
                pltpu.make_async_copy(c_ref, centers_ref, sems.at[n]),
                pltpu.make_async_copy(s_ref, scales_ref, sems.at[n + 1]),
            ]
            for copy in copies:
                copy.start()
            for copy in copies:
                copy.wait()


def on_device(kv_cache, valid_blocks):
    kind_count, layer_dev, user_count, per_dev, heads_dev, width = kv_cache.shape
    n, groups = lax.axis_size("seq"), lax.axis_size("groups")
    quarter = n // user_count
    part = per_dev // quarter
    kinds = kind_count * layer_dev * heads_dev
    kv = jnp.transpose(kv_cache, (0, 1, 4, 2, 3, 5)).reshape(kinds, user_count, per_dev, width)
    kv = pltpu.with_memory_space_constraint(kv, pltpu.HBM)
    blocks = pltpu.with_memory_space_constraint(valid_blocks, pltpu.HBM)
    vmem = pl.BlockSpec(memory_space=pltpu.VMEM)
    smem = pl.BlockSpec(memory_space=pltpu.SMEM)
    anywhere = pl.BlockSpec(memory_space=pl.ANY)
    hbm = pl.BlockSpec(memory_space=pltpu.HBM)
    table = (3, kinds, user_count, width)
    dma = pltpu.SemaphoreType.DMA
    small = jax.ShapeDtypeStruct((kinds, user_count, width), jnp.float32)
    whole = jax.ShapeDtypeStruct((kinds, n * part, width), jnp.bfloat16)
    early, centers, scales, inverse, lengths, choice = pl.pallas_call(
        functools.partial(gather, n, groups, quarter),
        out_shape=(
            whole, small, small, small,
            jax.ShapeDtypeStruct((user_count, width), jnp.int32),
            jax.ShapeDtypeStruct((1,), jnp.int32),
        ),
        in_specs=[hbm, hbm],
        out_specs=(vmem,) * 5 + (smem,),
        scratch_shapes=[
            pltpu.SMEM((groups, user_count), jnp.int32),
            pltpu.VMEM((kinds, user_count, per_dev, width), jnp.bfloat16),
            pltpu.VMEM((n,) + table, jnp.float32),
            pltpu.VMEM((2,) + table, jnp.float32),
            pltpu.VMEM(table, jnp.float32),
            dma, dma, dma, dma((n, kinds)), dma((n, kinds)), dma((kinds, 2)), dma((n, kinds, 2)),
            dma, dma((n,)), dma, dma, dma((n,)), dma, dma((groups,)), dma((groups,)),
            pltpu.SemaphoreType.REGULAR,
        ],
        compiler_params=pltpu.CompilerParams(
            collective_id=0, has_side_effects=True, vmem_limit_bytes=GRANT
        ),
        name="gather",
    )(blocks, kv)

    def branch(index):
        def run(lengths, centers, inverse):
            return pl.pallas_call(
                functools.partial(remainder, index, n, groups, quarter),
                out_shape=jax.ShapeDtypeStruct((kinds, (n // 2) * part, width), jnp.bfloat16),
                in_specs=[hbm, vmem, vmem, vmem],
                out_specs=vmem,
                scratch_shapes=[
                    dma((n, kinds)), dma((kinds,)), dma((kinds,)), dma((n // 2, kinds)),
                    pltpu.SemaphoreType.REGULAR,
                ],
                compiler_params=pltpu.CompilerParams(
                    collective_id=1 + index, has_side_effects=True, vmem_limit_bytes=GRANT
                ),
                name=f"remainder_{index}",
            )(kv, lengths, centers, inverse)

        return run

    late = lax.switch(
        choice[0],
        [branch(i) for i in range(len(classes(user_count)) ** groups)],
        lengths, centers, inverse,
    )
    out, centers, scales = pl.pallas_call(
        functools.partial(finish, n, part),
        out_shape=(whole, small, small),
        in_specs=[vmem] * 4,
        out_specs=(anywhere, anywhere, anywhere),
        scratch_shapes=[dma((n + 2,))],
        compiler_params=pltpu.CompilerParams(vmem_limit_bytes=GRANT),
        name="finish",
    )(early, late, centers, scales)

    def spread(x, middle):
        x = x.reshape(kind_count, layer_dev, heads_dev, *middle, width)
        return jnp.moveaxis(x, 2, -2)

    return (
        spread(out, (1, n * part)),
        spread(centers, (user_count,)),
        spread(scales, (user_count,)),
    )


def solution(mesh):
    in_specs = (P(None, "layer", "groups", "seq", "head", None), P("groups"))
    out_specs = (
        P(None, "layer", ("groups", "seq"), None, "head", None),
        P(None, "layer", "groups", "head", None),
        P(None, "layer", "groups", "head", None),
    )
    return jax.shard_map(
        on_device, mesh=mesh, in_specs=in_specs, out_specs=out_specs, check_vma=False
    )
```
